16 devices in a mesh: dp: 2 (over y, z), ctx: 8 (over x, core).
Axes of the slice: x: 4, y: 2, z: 1, core: 2. Of those that a mesh axis runs over, the one named last changes fastest.
The devices are a block of a 4x4x8 slice.
Arguments:
- x_chunk: bfloat16 [4096, 768], P(('dp', 'ctx')), parts along dimension 0
- cache_len: int32 [2], P('dp'), parts along dimension 0
- k_cache: bfloat16 [2, 32768, 12, 64], P(None, ('dp', 'ctx')), parts along dimension 1
- v_cache: bfloat16 [2, 32768, 12, 64], P(None, ('dp', 'ctx')), parts along dimension 1
- k_local: bfloat16 [2, 512, 12, 64], P(None, 'dp'), parts along dimension 1
- v_local: bfloat16 [2, 512, 12, 64], P(None, 'dp'), parts along dimension 1
- g_attn: bfloat16 [4, 768], replicated
- g_mlp: bfloat16 [4, 768], replicated
- w_q: bfloat16 [4, 768, 768], replicated
- w_k: bfloat16 [4, 768, 768], replicated
- w_v: bfloat16 [4, 768, 768], replicated
- w_o: bfloat16 [4, 768, 768], replicated
- w_gate: bfloat16 [4, 768, 3072], replicated
- w_up: bfloat16 [4, 768, 3072], replicated
- w_down: bfloat16 [4, 3072, 768], replicated
Outputs:
- output: bfloat16 [4096, 768], P(('dp', 'ctx')), parts along dimension 0
There are 2 independent parts. The reference program is written for one: setup_inputs(seed, part) draws one part's arguments, and reference() takes and returns one part's arrays. A program takes and returns all parts, laid end to end along the dimension named above; an argument that names none is the same for every part.
All inputs are finite; a program needn't handle non-finite values.
Results may differ from the reference program's by a relative error of at most 0.02.
Values are sent between devices in bfloat16 or wider.
A program may use at most 768 MiB of HBM per device.

```python
import math
import jax
import jax.numpy as jnp
from jax import lax

D_MODEL = 768
NUM_HEADS = 12
KV_HEADS = 12
HEAD_DIM = 64
WINDOW = 256
FF_DIM = 3072
SEQ_NEW = 2048
CACHE_SIZE = 16384
QUERY_ROWS = 128
NUM_PAIRS = 2
NORM_EPS = 1e-6


def draw_normal(rng_key, arr_shape, factor):
    return jax.random.normal(rng_key, arr_shape, jnp.float32) * factor


def setup_inputs(seed: int = 0, part: int = 0) -> dict:
    part_keys = jax.random.split(jax.random.fold_in(jax.random.key(seed), part), 6)
    shared_keys = jax.random.split(jax.random.key(seed + 1), 9)
    n_layers = 2 * NUM_PAIRS
    q_width = NUM_HEADS * HEAD_DIM
    kv_width = KV_HEADS * HEAD_DIM
    gain_local = math.log(max(WINDOW / 8.0, 2.0)) ** 0.25
    gain_global = math.log(max((CACHE_SIZE + SEQ_NEW) / 16.0, 2.0)) ** 0.25
    gain_base = jnp.tile(jnp.array([gain_local, gain_global], jnp.float32), NUM_PAIRS)
    cache_shape = (NUM_PAIRS, CACHE_SIZE, KV_HEADS, HEAD_DIM)
    local_shape = (NUM_PAIRS, WINDOW, KV_HEADS, HEAD_DIM)
    x_chunk = draw_normal(part_keys[0], (SEQ_NEW, D_MODEL), 1.0).astype(jnp.bfloat16)
    cache_len = jax.random.randint(part_keys[1], (1,), CACHE_SIZE // 2, CACHE_SIZE + 1, jnp.int32)
    k_cache = draw_normal(part_keys[2], cache_shape, gain_global).astype(jnp.bfloat16)
    v_cache = draw_normal(part_keys[3], cache_shape, gain_global).astype(jnp.bfloat16)
    k_local = draw_normal(part_keys[4], local_shape, gain_local).astype(jnp.bfloat16)
    v_local = draw_normal(part_keys[5], local_shape, gain_local).astype(jnp.bfloat16)
    g_attn = (gain_base[:, None] * (1.0 + draw_normal(shared_keys[0], (n_layers, D_MODEL), 0.2))).astype(jnp.bfloat16)
    g_mlp = (1.0 + draw_normal(shared_keys[1], (n_layers, D_MODEL), 0.2)).astype(jnp.bfloat16)
    w_q = draw_normal(shared_keys[2], (n_layers, D_MODEL, q_width), D_MODEL ** -0.5).astype(jnp.bfloat16)
    w_k = draw_normal(shared_keys[3], (n_layers, D_MODEL, kv_width), D_MODEL ** -0.5).astype(jnp.bfloat16)
    w_v = draw_normal(shared_keys[4], (n_layers, D_MODEL, kv_width), D_MODEL ** -0.5).astype(jnp.bfloat16)
    w_o = draw_normal(shared_keys[5], (n_layers, q_width, D_MODEL), q_width ** -0.5).astype(jnp.bfloat16)
    w_gate = draw_normal(shared_keys[6], (n_layers, D_MODEL, FF_DIM), D_MODEL ** -0.5).astype(jnp.bfloat16)
    w_up = draw_normal(shared_keys[7], (n_layers, D_MODEL, FF_DIM), D_MODEL ** -0.5).astype(jnp.bfloat16)
    w_down = draw_normal(shared_keys[8], (n_layers, FF_DIM, D_MODEL), FF_DIM ** -0.5).astype(jnp.bfloat16)
    return {'x_chunk': x_chunk, 'cache_len': cache_len, 'k_cache': k_cache, 'v_cache': v_cache,
            'k_local': k_local, 'v_local': v_local, 'g_attn': g_attn, 'g_mlp': g_mlp,
            'w_q': w_q, 'w_k': w_k, 'w_v': w_v, 'w_o': w_o,
            'w_gate': w_gate, 'w_up': w_up, 'w_down': w_down}


def rms_norm(rows_in, gain_vec):
    rows_f32 = rows_in.astype(jnp.float32)
    inv_rms = lax.rsqrt(jnp.mean(rows_f32 * rows_f32, axis=-1, keepdims=True) + NORM_EPS)
    return (rows_f32 * inv_rms * gain_vec.astype(jnp.float32)).astype(jnp.bfloat16)


def project(rows_in, weight):
    return jnp.dot(rows_in, weight, preferred_element_type=jnp.float32).astype(jnp.bfloat16)


def qkv_heads(normed, w_query, w_key, w_value):
    groups = NUM_HEADS // KV_HEADS
    queries = project(normed, w_query).reshape(SEQ_NEW, KV_HEADS, groups, HEAD_DIM)
    new_k = project(normed, w_key).reshape(SEQ_NEW, KV_HEADS, HEAD_DIM)
    new_v = project(normed, w_value).reshape(SEQ_NEW, KV_HEADS, HEAD_DIM)
    return queries, new_k, new_v


def attend(score_list, value_list):
    row_max = score_list[0].max(axis=-1)
    for part_scores in score_list[1:]:
        row_max = jnp.maximum(row_max, part_scores.max(axis=-1))
    row_sum = 0.0
    weighted = 0.0
    for part_scores, part_values in zip(score_list, value_list):
        part_probs = jnp.exp(part_scores - row_max[..., None])
        row_sum = row_sum + part_probs.sum(axis=-1)
        weighted = weighted + jnp.einsum('hgqk,khd->qhgd', part_probs.astype(jnp.bfloat16).astype(jnp.float32), part_values.astype(jnp.float32))
    return (weighted / jnp.transpose(row_sum, (2, 0, 1))[..., None]).astype(jnp.bfloat16)


def local_attention(queries, ext_k, ext_v):
    score_scale = HEAD_DIM ** -0.5
    rel_pos = jnp.arange(WINDOW + QUERY_ROWS)[None, :] - jnp.arange(QUERY_ROWS)[:, None]
    band_mask = (rel_pos > 0) & (rel_pos <= WINDOW)

    def one_block(block_idx):
        row_start = block_idx * QUERY_ROWS
        q_rows = lax.dynamic_slice_in_dim(queries, row_start, QUERY_ROWS, axis=0).astype(jnp.float32)
        k_rows = lax.dynamic_slice_in_dim(ext_k, row_start, WINDOW + QUERY_ROWS, axis=0)
        v_rows = lax.dynamic_slice_in_dim(ext_v, row_start, WINDOW + QUERY_ROWS, axis=0)
        scores = jnp.einsum('qhgd,khd->hgqk', q_rows, k_rows.astype(jnp.float32)) * score_scale
        scores = jnp.where(band_mask, scores, -jnp.inf)
        return attend([scores], [v_rows])

    blocks = lax.map(one_block, jnp.arange(SEQ_NEW // QUERY_ROWS))
    return blocks.reshape(SEQ_NEW, NUM_HEADS * HEAD_DIM)


def global_attention(queries, cache_k, cache_v, new_k, new_v, valid_len):
    score_scale = HEAD_DIM ** -0.5
    cache_mask = jnp.arange(CACHE_SIZE) < valid_len
    new_pos = jnp.arange(SEQ_NEW)
    cache_f32 = cache_k.astype(jnp.float32)
    new_f32 = new_k.astype(jnp.float32)

    def one_block(block_idx):
        row_start = block_idx * QUERY_ROWS
        q_rows = lax.dynamic_slice_in_dim(queries, row_start, QUERY_ROWS, axis=0).astype(jnp.float32)
        q_pos = row_start + jnp.arange(QUERY_ROWS)
        cache_scores = jnp.einsum('qhgd,khd->hgqk', q_rows, cache_f32) * score_scale
        cache_scores = jnp.where(cache_mask, cache_scores, -jnp.inf)
        new_scores = jnp.einsum('qhgd,khd->hgqk', q_rows, new_f32) * score_scale
        new_scores = jnp.where(new_pos[None, :] <= q_pos[:, None], new_scores, -jnp.inf)
        return attend([cache_scores, new_scores], [cache_v, new_v])

    blocks = lax.map(one_block, jnp.arange(SEQ_NEW // QUERY_ROWS))
    return blocks.reshape(SEQ_NEW, NUM_HEADS * HEAD_DIM)


def add_residual(hidden, attn_out, w_out):
    return (hidden.astype(jnp.float32) + jnp.dot(attn_out, w_out, preferred_element_type=jnp.float32)).astype(jnp.bfloat16)


def mlp_block(hidden, gain_vec, w_gate, w_up, w_down):
    normed = rms_norm(hidden, gain_vec)
    gate_pre = jnp.dot(normed, w_gate, preferred_element_type=jnp.float32)
    up_pre = jnp.dot(normed, w_up, preferred_element_type=jnp.float32)
    act_bf16 = (jax.nn.gelu(gate_pre, approximate=True) * up_pre).astype(jnp.bfloat16)
    return (hidden.astype(jnp.float32) + jnp.dot(act_bf16, w_down, preferred_element_type=jnp.float32)).astype(jnp.bfloat16)


def reference(x_chunk, cache_len, k_cache, v_cache, k_local, v_local, g_attn, g_mlp, w_q, w_k, w_v, w_o, w_gate, w_up, w_down):
    hidden = x_chunk
    for pair_idx in range(NUM_PAIRS):
        layer_idx = 2 * pair_idx
        queries, new_k, new_v = qkv_heads(rms_norm(hidden, g_attn[layer_idx]), w_q[layer_idx], w_k[layer_idx], w_v[layer_idx])
        ext_k = jnp.concatenate([k_local[pair_idx], new_k], axis=0)
        ext_v = jnp.concatenate([v_local[pair_idx], new_v], axis=0)
        attn_out = local_attention(queries, ext_k, ext_v)
        hidden = add_residual(hidden, attn_out, w_o[layer_idx])
        hidden = mlp_block(hidden, g_mlp[layer_idx], w_gate[layer_idx], w_up[layer_idx], w_down[layer_idx])
        layer_idx = 2 * pair_idx + 1
        queries, new_k, new_v = qkv_heads(rms_norm(hidden, g_attn[layer_idx]), w_q[layer_idx], w_k[layer_idx], w_v[layer_idx])
        attn_out = global_attention(queries, k_cache[pair_idx], v_cache[pair_idx], new_k, new_v, cache_len[0])
        hidden = add_residual(hidden, attn_out, w_o[layer_idx])
        hidden = mlp_block(hidden, g_mlp[layer_idx], w_gate[layer_idx], w_up[layer_idx], w_down[layer_idx])
    return hidden
```

```python
import functools

import jax
import jax.numpy as jnp
from jax import lax
from jax.experimental import pallas as pl
from jax.experimental.pallas import tpu as pltpu
from jax.sharding import PartitionSpec as P, NamedSharding

NORM_EPS = 1e-6


def rms_norm(rows_in, gain_vec):
    rows_f32 = rows_in.astype(jnp.float32)
    inv_rms = lax.rsqrt(jnp.mean(rows_f32 * rows_f32, axis=-1, keepdims=True) + NORM_EPS)
    return (rows_f32 * inv_rms * gain_vec.astype(jnp.float32)).astype(jnp.bfloat16)


def project(rows_in, weight):
    return jnp.dot(rows_in, weight, preferred_element_type=jnp.float32).astype(jnp.bfloat16)


def qkv_heads(normed, w_query, w_key, w_value, kv_heads, head_dim):
    lead_dims = normed.shape[:-1]
    groups = w_query.shape[-1] // (kv_heads * head_dim)
    queries = project(normed, w_query).reshape(lead_dims + (kv_heads, groups, head_dim))
    new_k = project(normed, w_key).reshape(lead_dims + (kv_heads, head_dim))
    new_v = project(normed, w_value).reshape(lead_dims + (kv_heads, head_dim))
    return queries, new_k, new_v


def add_residual(hidden, attn_out, w_out):
    return (hidden.astype(jnp.float32) + jnp.dot(attn_out, w_out, preferred_element_type=jnp.float32)).astype(jnp.bfloat16)


def mlp_block(hidden, gain_vec, w_gate, w_up, w_down):
    normed = rms_norm(hidden, gain_vec)
    gate_pre = jnp.dot(normed, w_gate, preferred_element_type=jnp.float32)
    up_pre = jnp.dot(normed, w_up, preferred_element_type=jnp.float32)
    act_bf16 = (jax.nn.gelu(gate_pre, approximate=True) * up_pre).astype(jnp.bfloat16)
    return (hidden.astype(jnp.float32) + jnp.dot(act_bf16, w_down, preferred_element_type=jnp.float32)).astype(jnp.bfloat16)


def band_attention(queries, ext_k, ext_v):
    n_rows, kv_heads, groups, head_dim = queries.shape
    window = ext_k.shape[0] - n_rows
    blocks = n_rows // window
    score_scale = head_dim ** -0.5
    q_blocks = queries.reshape(blocks, window, kv_heads, groups, head_dim)
    k_blocks = ext_k.reshape(blocks + 1, window, kv_heads, head_dim)
    v_blocks = ext_v.reshape(blocks + 1, window, kv_heads, head_dim)
    row_ids = lax.broadcasted_iota(jnp.int32, (window, window), 0)
    col_ids = lax.broadcasted_iota(jnp.int32, (window, window), 1)
    prev_scores = jnp.einsum('bqhgd,bkhd->bhgqk', q_blocks, k_blocks[:-1], preferred_element_type=jnp.float32) * score_scale
    prev_scores = jnp.where(col_ids > row_ids, prev_scores, -jnp.inf)
    own_scores = jnp.einsum('bqhgd,bkhd->bhgqk', q_blocks, k_blocks[1:], preferred_element_type=jnp.float32) * score_scale
    own_scores = jnp.where(col_ids <= row_ids, own_scores, -jnp.inf)
    row_max = jnp.maximum(prev_scores.max(axis=-1), own_scores.max(axis=-1))[..., None]
    prev_probs = jnp.exp(prev_scores - row_max)
    own_probs = jnp.exp(own_scores - row_max)
    row_sum = prev_probs.sum(axis=-1) + own_probs.sum(axis=-1)
    weighted = (jnp.einsum('bhgqk,bkhd->bqhgd', prev_probs.astype(jnp.bfloat16), v_blocks[:-1], preferred_element_type=jnp.float32)
                + jnp.einsum('bhgqk,bkhd->bqhgd', own_probs.astype(jnp.bfloat16), v_blocks[1:], preferred_element_type=jnp.float32))
    out_rows = weighted / jnp.transpose(row_sum, (0, 3, 1, 2))[..., None]
    return out_rows.astype(jnp.bfloat16).reshape(n_rows, kv_heads * groups * head_dim)


LOG2E = 1.4426950408889634
NEG = -1e38
MESH_ID = pl.DeviceIdType.MESH
ROWS = 256
CHUNK = 256
STATS = 8


def slot_of(step):
    unit = step // 2
    return unit + unit // 2 - 2 * (unit // 3), step % 2


def global_kernel(n_chips, pair, len_ref, q_ref, k_ref, v_ref, kc_ref, vc_ref, out_ref,
                  k_own, v_own, k_sib, v_sib, kn_sib, vn_sib, q_all, k_ext, scores, part, parts,
                  own_sem, sib_send, sib_recv, q_send, q_recv, o_send, o_recv):
    heads, head_dim, slots = k_own.shape
    n_slots = 2 * n_chips
    me = lax.axis_index('ctx')
    chip, core = me // 2, me % 2
    first_head = heads * core
    other_head = heads * (1 - core)
    sibling = {'ctx': 2 * chip + (1 - core)}
    n_new = 2 * ROWS
    n_keys = 2 * slots + n_new

    barrier = pltpu.get_barrier_semaphore()
    for step in range(1, n_slots):
        pl.semaphore_signal(barrier, inc=1, device_id={'ctx': (me + step) % n_slots}, device_id_type=MESH_ID)

    def own_copies(head):
        return (pltpu.make_async_copy(kc_ref.at[pair, first_head + head], k_own.at[head], own_sem.at[0, head]),
                pltpu.make_async_copy(vc_ref.at[pair, first_head + head], v_own.at[head], own_sem.at[1, head]))

    def sib_copies(head):
        pairs = ((kc_ref.at[pair, other_head + head], k_sib.at[head]),
                 (vc_ref.at[pair, other_head + head], v_sib.at[head]),
                 (k_ref.at[other_head + head], kn_sib.at[head]),
                 (v_ref.at[other_head + head], vn_sib.at[head]))
        return [pltpu.make_async_remote_copy(src_ref=src, dst_ref=dst, send_sem=sib_send.at[which, head],
                                             recv_sem=sib_recv.at[which, head], device_id=sibling, device_id_type=MESH_ID)
                for which, (src, dst) in enumerate(pairs)]

    def target(dist, flip):
        return {'ctx': 2 * ((chip + dist) % n_chips) + (core + flip) % 2}

    def q_copy(dist, flip, head):
        slot = 2 * dist + flip
        their_head = heads * ((core + flip) % 2) + head
        return pltpu.make_async_remote_copy(src_ref=q_ref.at[their_head], dst_ref=q_all.at[slot, head],
                                            send_sem=q_send.at[slot, head], recv_sem=q_recv.at[slot, head],
                                            device_id=target(dist, flip), device_id_type=MESH_ID)

    def o_copy(dist, flip, head):
        slot = 2 * dist + flip
        owner = {'ctx': 2 * ((chip + n_chips - dist) % n_chips) + (core + flip) % 2}
        return pltpu.make_async_remote_copy(src_ref=part.at[slot, head], dst_ref=parts.at[slot, head],
                                            send_sem=o_send.at[slot, head], recv_sem=o_recv.at[slot, head],
                                            device_id=owner, device_id_type=MESH_ID)

    def start_own(head, carry):
        for copy in own_copies(head):
            copy.start()
        q_all[0, head] = q_ref[first_head + head]
        return carry

    lax.fori_loop(0, heads, start_own, 0)
    pl.semaphore_wait(barrier, n_slots - 1)

    def start_head(head, carry):
        for copy in sib_copies(head):
            copy.start()

        def start_q(step, inner):
            dist, flip = slot_of(step)
            q_copy(dist, flip, head).start()
            return inner

        lax.fori_loop(1, n_slots, start_q, 0)
        return carry

    lax.fori_loop(0, heads, start_head, 0)

    valid = len_ref[0]

    def prepare(head):
        for copy in own_copies(head):
            copy.wait()
        for copy in sib_copies(head):
            copy.wait_recv()
        width = 512
        row = lax.broadcasted_iota(jnp.int32, (head_dim, width), 0)
        col = lax.broadcasted_iota(jnp.int32, (head_dim, width), 1)
        for begin in range(0, n_keys, width):
            if begin < 2 * slots:
                source = k_own if begin < slots else k_sib
                at = begin % slots
                tile = source[head, :, at:at + width]
                device = me if begin < slots else 2 * chip + (1 - core)
                bias = jnp.where((row == 0) & (device * slots + at + col >= valid), NEG, 0.0)
            else:
                tile = jnp.concatenate([k_ref[first_head + head], kn_sib[head]], axis=1)
                bias = jnp.where((row == 1) & (col < ROWS) | (row == 2) & (col >= ROWS), 1.0, 0.0)
            buf = head % 2
            k_ext[buf, begin:begin + width, 0:2 * head_dim] = jnp.concatenate([tile, tile], axis=0).T
            k_ext[buf, begin:begin + width, 2 * head_dim:] = jnp.concatenate([tile, bias.astype(jnp.bfloat16)], axis=0).T

    def query_columns(head, dist, flip):
        slot = 2 * dist + flip
        full = q_all[slot, head].astype(jnp.float32) * (LOG2E * head_dim ** -0.5)
        high = full.astype(jnp.bfloat16)
        rest = full - high.astype(jnp.float32)
        middle = rest.astype(jnp.bfloat16)
        low = (rest - middle.astype(jnp.float32)).astype(jnp.bfloat16)
        q_dev = 2 * ((chip + n_chips - dist) % n_chips) + (core + flip) % 2
        row = lax.broadcasted_iota(jnp.int32, (head_dim, ROWS), 0)
        hide_own = jnp.where(q_dev < me, NEG, 0.0)
        hide_sib = jnp.where(q_dev < 2 * chip + (1 - core), NEG, 0.0)
        mask = jnp.where(row == 0, 1.0, jnp.where(row == 1, hide_own, jnp.where(row == 2, hide_sib, 0.0)))
        return jnp.concatenate([high, middle, low, mask.astype(jnp.bfloat16)], axis=0), q_dev

    def score_chunk(buf, columns, q_dev, begin, top):
        keys = pl.ds(begin, CHUNK)
        block = jnp.dot(k_ext[buf, keys, :], columns, preferred_element_type=jnp.float32)
        if begin >= 2 * slots:
            device = me if begin < 2 * slots + ROWS else 2 * chip + (1 - core)
            ahead = lax.broadcasted_iota(jnp.int32, (CHUNK, ROWS), 0) - lax.broadcasted_iota(jnp.int32, (CHUNK, ROWS), 1)
            block = jnp.where(ahead <= jnp.where(q_dev == device, 0, ROWS), block, NEG)
        scores[keys, :] = block
        return jnp.maximum(top, jnp.max(block.reshape(CHUNK // 8, 8, ROWS), axis=0))

    def value_chunk(head, base, begin, total, weighted):
        keys = pl.ds(begin, CHUNK)
        probs = jnp.exp2(scores[keys, :] - base)
        total = total + jnp.sum(probs.reshape(CHUNK // 8, 8, ROWS), axis=0)
        if begin < slots:
            values = v_own[head, :, begin:begin + CHUNK]
        elif begin < 2 * slots:
            values = v_sib[head, :, begin - slots:begin - slots + CHUNK]
        elif begin < 2 * slots + ROWS:
            values = v_ref[first_head + head]
        else:
            values = vn_sib[head]
        return total, weighted + jnp.dot(values, probs.astype(jnp.bfloat16), preferred_element_type=jnp.float32)

    no_top = jnp.full((8, ROWS), NEG, jnp.float32)

    prepare(0)
    columns, q_dev = query_columns(0, 0, 0)
    top = no_top
    for begin in range(0, n_keys, CHUNK):
        top = score_chunk(0, columns, q_dev, begin, top)

    def one_head(head, top):
        next_head = jnp.minimum(head + 1, heads - 1)

        @pl.when(head < heads - 1)
        def _():
            prepare(next_head)

        def one_step(step, top):
            dist, flip = slot_of(step)
            slot = 2 * dist + flip
            after = (step + 1) % n_slots
            dist_n, flip_n = slot_of(after)
            head_n = jnp.where(step == n_slots - 1, next_head, head)

            @pl.when(after > 0)
            def _():
                q_copy(dist_n, flip_n, head).wait_recv()

            columns, q_dev = query_columns(head_n, dist_n, flip_n)
            base = jnp.max(top, axis=0, keepdims=True)
            total = jnp.zeros((8, ROWS), jnp.float32)
            weighted = jnp.zeros((head_dim, ROWS), jnp.float32)
            new_top = no_top
            for begin in range(0, n_keys, CHUNK):
                total, weighted = value_chunk(head, base, begin, total, weighted)
                new_top = score_chunk(head_n % 2, columns, q_dev, begin, new_top)
            row = lax.broadcasted_iota(jnp.int32, (STATS, ROWS), 0)
            total = jnp.sum(total, axis=0, keepdims=True)
            part[slot, head, 0:head_dim, :] = weighted
            part[slot, head, head_dim:, :] = jnp.where(row == 0, base, total)

            @pl.when(step > 0)
            def _():
                o_copy(dist, flip, head).start()

            return new_top

        return lax.fori_loop(0, n_slots, one_step, top)

    lax.fori_loop(0, heads, one_head, top)

    def merge(head, carry):
        for flip in range(2):
            found = []
            for dist in range(n_chips):
                slot = 2 * dist + flip
                if slot == 0:
                    found.append((part[0, head, 0:head_dim, :], part[0, head, head_dim:head_dim + 1, :],
                                  part[0, head, head_dim + 1:head_dim + 2, :]))
                else:
                    o_copy(dist, flip, head).wait_recv()
                    found.append((parts[slot, head, 0:head_dim, :], parts[slot, head, head_dim:head_dim + 1, :],
                                  parts[slot, head, head_dim + 1:head_dim + 2, :]))
            peak = functools.reduce(jnp.maximum, [base for _, base, _ in found])
            scaled = [(weighted, total, jnp.exp2(base - peak)) for weighted, base, total in found]
            upper = sum(weighted * factor for weighted, _, factor in scaled)
            lower = sum(total * factor for _, total, factor in scaled)
            out_ref[heads * ((core + flip) % 2) + head] = (upper / lower).astype(jnp.bfloat16)
        return carry

    lax.fori_loop(0, heads, merge, 0)

    def finish(head, carry):
        for copy in sib_copies(head):
            copy.wait_send()

        def finish_step(step, inner):
            dist, flip = slot_of(step)
            q_copy(dist, flip, head).wait_send()
            o_copy(dist, flip, head).wait_send()
            return inner

        lax.fori_loop(1, n_slots, finish_step, 0)
        return carry

    lax.fori_loop(0, heads, finish, 0)


def global_attention(pair, n_dev, valid_len, queries, new_k, new_v, cache_k, cache_v):
    all_heads, head_dim, rows = queries.shape
    heads = all_heads // 2
    slots = cache_k.shape[-1]
    n_keys = 2 * (slots + rows)
    vmem = pl.BlockSpec(memory_space=pltpu.VMEM)
    bf16, f32 = jnp.bfloat16, jnp.float32
    return pl.pallas_call(
        functools.partial(global_kernel, n_dev // 2, pair),
        out_shape=jax.ShapeDtypeStruct((all_heads, head_dim, rows), bf16),
        in_specs=[pl.BlockSpec(memory_space=pltpu.SMEM), vmem, vmem, vmem,
                  pl.BlockSpec(memory_space=pl.ANY), pl.BlockSpec(memory_space=pl.ANY)],
        out_specs=vmem,
        scratch_shapes=[
            pltpu.VMEM((heads, head_dim, slots), bf16), pltpu.VMEM((heads, head_dim, slots), bf16),
            pltpu.VMEM((heads, head_dim, slots), bf16), pltpu.VMEM((heads, head_dim, slots), bf16),
            pltpu.VMEM((heads, head_dim, rows), bf16), pltpu.VMEM((heads, head_dim, rows), bf16),
            pltpu.VMEM((n_dev, heads, head_dim, rows), bf16),
            pltpu.VMEM((2, n_keys, 4 * head_dim), bf16),
            pltpu.VMEM((n_keys, rows), f32),
            pltpu.VMEM((n_dev, heads, head_dim + STATS, rows), f32),
            pltpu.VMEM((n_dev, heads, head_dim + STATS, rows), f32),
            pltpu.SemaphoreType.DMA((2, heads)),
            pltpu.SemaphoreType.DMA((4, heads)), pltpu.SemaphoreType.DMA((4, heads)),
            pltpu.SemaphoreType.DMA((n_dev, heads)), pltpu.SemaphoreType.DMA((n_dev, heads)),
            pltpu.SemaphoreType.DMA((n_dev, heads)), pltpu.SemaphoreType.DMA((n_dev, heads)),
        ],
        compiler_params=pltpu.CompilerParams(collective_id=pair, has_side_effects=True, vmem_limit_bytes=56 * 2 ** 20),
        name='global_attn_%d' % pair,
    )(valid_len, queries, new_k, new_v, cache_k, cache_v)


def solution(mesh):
    ctx_size = mesh.shape['ctx']
    shift_pairs = [(src_dev, src_dev + 1) for src_dev in range(ctx_size - 1)]
    row_spec = P(('dp', 'ctx'), None)
    cache_spec = P(None, ('dp', 'ctx'), None, None)
    local_spec = P(None, 'dp', None, None)
    in_specs = (row_spec, P('dp'), cache_spec, cache_spec, local_spec, local_spec) + (P(),) * 9

    def device_step(x_rows, cache_len, k_cache, v_cache, k_local, v_local, g_attn, g_mlp, w_q, w_k, w_v, w_o, w_gate, w_up, w_down):
        dev_idx = lax.axis_index('ctx')
        is_first = dev_idx == 0
        n_rows = x_rows.shape[0]
        window = k_local.shape[1]
        kv_heads = k_local.shape[2]
        head_dim = k_local.shape[3]
        cache_k_t = jnp.transpose(k_cache, (0, 2, 3, 1))
        cache_v_t = jnp.transpose(v_cache, (0, 2, 3, 1))
        hidden = x_rows
        for pair_idx in range(k_cache.shape[0]):
            layer_idx = 2 * pair_idx
            queries, new_k, new_v = qkv_heads(rms_norm(hidden, g_attn[layer_idx]), w_q[layer_idx], w_k[layer_idx], w_v[layer_idx], kv_heads, head_dim)
            halo_k = lax.ppermute(new_k[n_rows - window:], 'ctx', shift_pairs)
            halo_v = lax.ppermute(new_v[n_rows - window:], 'ctx', shift_pairs)
            halo_k = jnp.where(is_first, k_local[pair_idx], halo_k)
            halo_v = jnp.where(is_first, v_local[pair_idx], halo_v)
            attn_out = band_attention(queries, jnp.concatenate([halo_k, new_k], axis=0), jnp.concatenate([halo_v, new_v], axis=0))
            hidden = add_residual(hidden, attn_out, w_o[layer_idx])
            hidden = mlp_block(hidden, g_mlp[layer_idx], w_gate[layer_idx], w_up[layer_idx], w_down[layer_idx])
            layer_idx = 2 * pair_idx + 1
            normed = rms_norm(hidden, g_attn[layer_idx])
            queries, new_k, new_v = [
                lax.dot_general(weight[layer_idx], normed, (((0,), (1,)), ((), ())), preferred_element_type=jnp.float32)
                .astype(jnp.bfloat16).reshape(kv_heads, head_dim, n_rows) for weight in (w_q, w_k, w_v)]
            attn_t = global_attention(pair_idx, ctx_size, cache_len, queries, new_k, new_v, cache_k_t, cache_v_t)
            attn_out = attn_t.reshape(kv_heads * head_dim, n_rows).T
            hidden = add_residual(hidden, attn_out, w_o[layer_idx])
            hidden = mlp_block(hidden, g_mlp[layer_idx], w_gate[layer_idx], w_up[layer_idx], w_down[layer_idx])
        return hidden

    return jax.shard_map(device_step, mesh=mesh, in_specs=in_specs, out_specs=row_spec, check_vma=False)
```

```python
import functools

import jax
import jax.numpy as jnp
from jax import lax
from jax.experimental import pallas as pl
from jax.experimental.pallas import tpu as pltpu
from jax.sharding import PartitionSpec as P

NORM_EPS = 1e-6
LOG2E = 1.4426950408889634
NEG = -1e38
MESH_ID = pl.DeviceIdType.MESH
ROWS = 256
CHUNK = 256
STATS = 8


def slot_of(step):
    unit = step // 2
    return unit + unit // 2 - 2 * (unit // 3), step % 2


def global_kernel(n_chips, pair, len_ref, q_ref, k_ref, v_ref, kc_ref, vc_ref, out_ref,
                  k_own, v_own, k_sib, v_sib, kn_sib, vn_sib, q_all, k_ext, scores, part, parts,
                  own_sem, sib_send, sib_recv, q_send, q_recv, o_send, o_recv):
    heads, head_dim, slots = k_own.shape
    n_slots = 2 * n_chips
    me = lax.axis_index('ctx')
    chip, core = me // 2, me % 2
    first_head = heads * core
    other_head = heads * (1 - core)
    sibling = {'ctx': 2 * chip + (1 - core)}
    n_new = 2 * ROWS
    n_keys = 2 * slots + n_new

    barrier = pltpu.get_barrier_semaphore()
    for step in range(1, n_slots):
        pl.semaphore_signal(barrier, inc=1, device_id={'ctx': (me + step) % n_slots}, device_id_type=MESH_ID)

    def own_copies(head):
        return (pltpu.make_async_copy(kc_ref.at[pair, first_head + head], k_own.at[head], own_sem.at[0, head]),
                pltpu.make_async_copy(vc_ref.at[pair, first_head + head], v_own.at[head], own_sem.at[1, head]))

    def sib_copies(head):
        pairs = ((kc_ref.at[pair, other_head + head], k_sib.at[head]),
                 (vc_ref.at[pair, other_head + head], v_sib.at[head]),
                 (k_ref.at[other_head + head], kn_sib.at[head]),
                 (v_ref.at[other_head + head], vn_sib.at[head]))
        return [pltpu.make_async_remote_copy(src_ref=src, dst_ref=dst, send_sem=sib_send.at[which, head],
                                             recv_sem=sib_recv.at[which, head], device_id=sibling, device_id_type=MESH_ID)
                for which, (src, dst) in enumerate(pairs)]

    def target(dist, flip):
        return {'ctx': 2 * ((chip + dist) % n_chips) + (core + flip) % 2}

    def q_copy(dist, flip, head):
        slot = 2 * dist + flip
        their_head = heads * ((core + flip) % 2) + head
        return pltpu.make_async_remote_copy(src_ref=q_ref.at[their_head], dst_ref=q_all.at[slot, head],
                                            send_sem=q_send.at[slot, head], recv_sem=q_recv.at[slot, head],
                                            device_id=target(dist, flip), device_id_type=MESH_ID)

    def o_copy(dist, flip, head):
        slot = 2 * dist + flip
        owner = {'ctx': 2 * ((chip + n_chips - dist) % n_chips) + (core + flip) % 2}
        return pltpu.make_async_remote_copy(src_ref=part.at[slot, head], dst_ref=parts.at[slot, head],
                                            send_sem=o_send.at[slot, head], recv_sem=o_recv.at[slot, head],
                                            device_id=owner, device_id_type=MESH_ID)

    def start_own(head, carry):
        for copy in own_copies(head):
            copy.start()
        q_all[0, head] = q_ref[first_head + head]
        return carry

    lax.fori_loop(0, heads, start_own, 0)
    pl.semaphore_wait(barrier, n_slots - 1)

    def start_head(head, carry):
        for copy in sib_copies(head):
            copy.start()

        def start_q(step, inner):
            dist, flip = slot_of(step)
            q_copy(dist, flip, head).start()
            return inner

        lax.fori_loop(1, n_slots, start_q, 0)
        return carry

    lax.fori_loop(0, heads, start_head, 0)

    valid = len_ref[0]

    def prepare(head):
        for copy in own_copies(head):
            copy.wait()
        for copy in sib_copies(head):
            copy.wait_recv()
        width = 512
        row = lax.broadcasted_iota(jnp.int32, (head_dim, width), 0)
        col = lax.broadcasted_iota(jnp.int32, (head_dim, width), 1)
        for begin in range(0, n_keys, width):
            if begin < 2 * slots:
                source = k_own if begin < slots else k_sib
                at = begin % slots
                tile = source[head, :, at:at + width]
                device = me if begin < slots else 2 * chip + (1 - core)
                bias = jnp.where((row == 0) & (device * slots + at + col >= valid), NEG, 0.0)
            else:
                tile = jnp.concatenate([k_ref[first_head + head], kn_sib[head]], axis=1)
                bias = jnp.where((row == 1) & (col < ROWS) | (row == 2) & (col >= ROWS), 1.0, 0.0)
            buf = head % 2
            k_ext[buf, begin:begin + width, 0:2 * head_dim] = jnp.concatenate([tile, tile], axis=0).T
            k_ext[buf, begin:begin + width, 2 * head_dim:] = jnp.concatenate([tile, bias.astype(jnp.bfloat16)], axis=0).T

    def query_columns(head, dist, flip):
        slot = 2 * dist + flip
        full = q_all[slot, head].astype(jnp.float32) * (LOG2E * head_dim ** -0.5)
        high = full.astype(jnp.bfloat16)
        rest = full - high.astype(jnp.float32)
        middle = rest.astype(jnp.bfloat16)
        low = (rest - middle.astype(jnp.float32)).astype(jnp.bfloat16)
        q_dev = 2 * ((chip + n_chips - dist) % n_chips) + (core + flip) % 2
        row = lax.broadcasted_iota(jnp.int32, (head_dim, ROWS), 0)
        hide_own = jnp.where(q_dev < me, NEG, 0.0)
        hide_sib = jnp.where(q_dev < 2 * chip + (1 - core), NEG, 0.0)
        mask = jnp.where(row == 0, 1.0, jnp.where(row == 1, hide_own, jnp.where(row == 2, hide_sib, 0.0)))
        return jnp.concatenate([high, middle, low, mask.astype(jnp.bfloat16)], axis=0), q_dev

    def score_chunk(buf, columns, q_dev, begin, top):
        keys = pl.ds(begin, CHUNK)
        block = jnp.dot(k_ext[buf, keys, :], columns, preferred_element_type=jnp.float32)
        if begin >= 2 * slots:
            device = me if begin < 2 * slots + ROWS else 2 * chip + (1 - core)
            ahead = lax.broadcasted_iota(jnp.int32, (CHUNK, ROWS), 0) - lax.broadcasted_iota(jnp.int32, (CHUNK, ROWS), 1)
            block = jnp.where(ahead <= jnp.where(q_dev == device, 0, ROWS), block, NEG)
        scores[keys, :] = block
        return jnp.maximum(top, jnp.max(block.reshape(CHUNK // 8, 8, ROWS), axis=0))

    def value_chunk(head, base, begin, total, weighted):
        keys = pl.ds(begin, CHUNK)
        probs = jnp.exp2(scores[keys, :] - base)
        total = total + jnp.sum(probs.reshape(CHUNK // 8, 8, ROWS), axis=0)
        if begin < slots:
            values = v_own[head, :, begin:begin + CHUNK]
        elif begin < 2 * slots:
            values = v_sib[head, :, begin - slots:begin - slots + CHUNK]
        elif begin < 2 * slots + ROWS:
            values = v_ref[first_head + head]
        else:
            values = vn_sib[head]
        return total, weighted + jnp.dot(values, probs.astype(jnp.bfloat16), preferred_element_type=jnp.float32)

    no_top = jnp.full((8, ROWS), NEG, jnp.float32)

    prepare(0)
    columns, q_dev = query_columns(0, 0, 0)
    top = no_top
    for begin in range(0, n_keys, CHUNK):
        top = score_chunk(0, columns, q_dev, begin, top)

    def one_head(head, top):
        next_head = jnp.minimum(head + 1, heads - 1)

        @pl.when(head < heads - 1)
        def _():
            prepare(next_head)

        def one_step(step, top):
            dist, flip = slot_of(step)
            slot = 2 * dist + flip
            after = (step + 1) % n_slots
            dist_n, flip_n = slot_of(after)
            head_n = jnp.where(step == n_slots - 1, next_head, head)

            @pl.when(after > 0)
            def _():
                q_copy(dist_n, flip_n, head).wait_recv()

            columns, q_dev = query_columns(head_n, dist_n, flip_n)
            base = jnp.max(top, axis=0, keepdims=True)
            total = jnp.zeros((8, ROWS), jnp.float32)
            weighted = jnp.zeros((head_dim, ROWS), jnp.float32)
            new_top = no_top
            for begin in range(0, n_keys, CHUNK):
                total, weighted = value_chunk(head, base, begin, total, weighted)
                new_top = score_chunk(head_n % 2, columns, q_dev, begin, new_top)
            row = lax.broadcasted_iota(jnp.int32, (STATS, ROWS), 0)
            total = jnp.sum(total, axis=0, keepdims=True)
            part[slot, head, 0:head_dim, :] = weighted
            part[slot, head, head_dim:, :] = jnp.where(row == 0, base, total)

            @pl.when(step > 0)
            def _():
                o_copy(dist, flip, head).start()

            return new_top

        return lax.fori_loop(0, n_slots, one_step, top)

    lax.fori_loop(0, heads, one_head, top)

    def merge(head, carry):
        for flip in range(2):
            found = []
            for dist in range(n_chips):
                slot = 2 * dist + flip
                if slot == 0:
                    found.append((part[0, head, 0:head_dim, :], part[0, head, head_dim:head_dim + 1, :],
                                  part[0, head, head_dim + 1:head_dim + 2, :]))
                else:
                    o_copy(dist, flip, head).wait_recv()
                    found.append((parts[slot, head, 0:head_dim, :], parts[slot, head, head_dim:head_dim + 1, :],
                                  parts[slot, head, head_dim + 1:head_dim + 2, :]))
            peak = functools.reduce(jnp.maximum, [base for _, base, _ in found])
            scaled = [(weighted, total, jnp.exp2(base - peak)) for weighted, base, total in found]
            upper = sum(weighted * factor for weighted, _, factor in scaled)
            lower = sum(total * factor for _, total, factor in scaled)
            out_ref[heads * ((core + flip) % 2) + head] = (upper / lower).astype(jnp.bfloat16)
        return carry

    lax.fori_loop(0, heads, merge, 0)

    def finish(head, carry):
        for copy in sib_copies(head):
            copy.wait_send()

        def finish_step(step, inner):
            dist, flip = slot_of(step)
            q_copy(dist, flip, head).wait_send()
            o_copy(dist, flip, head).wait_send()
            return inner

        lax.fori_loop(1, n_slots, finish_step, 0)
        return carry

    lax.fori_loop(0, heads, finish, 0)


def global_attention(pair, n_dev, valid_len, queries, new_k, new_v, cache_k, cache_v):
    all_heads, head_dim, rows = queries.shape
    heads = all_heads // 2
    slots = cache_k.shape[-1]
    n_keys = 2 * (slots + rows)
    vmem = pl.BlockSpec(memory_space=pltpu.VMEM)
    bf16, f32 = jnp.bfloat16, jnp.float32
    return pl.pallas_call(
        functools.partial(global_kernel, n_dev // 2, pair),
        out_shape=jax.ShapeDtypeStruct((all_heads, head_dim, rows), bf16),
        in_specs=[pl.BlockSpec(memory_space=pltpu.SMEM), vmem, vmem, vmem,
                  pl.BlockSpec(memory_space=pl.ANY), pl.BlockSpec(memory_space=pl.ANY)],
        out_specs=vmem,
        scratch_shapes=[
            pltpu.VMEM((heads, head_dim, slots), bf16), pltpu.VMEM((heads, head_dim, slots), bf16),
            pltpu.VMEM((heads, head_dim, slots), bf16), pltpu.VMEM((heads, head_dim, slots), bf16),
            pltpu.VMEM((heads, head_dim, rows), bf16), pltpu.VMEM((heads, head_dim, rows), bf16),
            pltpu.VMEM((n_dev, heads, head_dim, rows), bf16),
            pltpu.VMEM((2, n_keys, 4 * head_dim), bf16),
            pltpu.VMEM((n_keys, rows), f32),
            pltpu.VMEM((n_dev, heads, head_dim + STATS, rows), f32),
            pltpu.VMEM((n_dev, heads, head_dim + STATS, rows), f32),
            pltpu.SemaphoreType.DMA((2, heads)),
            pltpu.SemaphoreType.DMA((4, heads)), pltpu.SemaphoreType.DMA((4, heads)),
            pltpu.SemaphoreType.DMA((n_dev, heads)), pltpu.SemaphoreType.DMA((n_dev, heads)),
            pltpu.SemaphoreType.DMA((n_dev, heads)), pltpu.SemaphoreType.DMA((n_dev, heads)),
        ],
        compiler_params=pltpu.CompilerParams(collective_id=pair, has_side_effects=True, vmem_limit_bytes=56 * 2 ** 20),
        name='global_attn_%d' % pair,
    )(valid_len, queries, new_k, new_v, cache_k, cache_v)


def rms_rows(rows_in, gain_row):
    rows_f32 = rows_in.astype(jnp.float32)
    inv_rms = lax.rsqrt(jnp.mean(rows_f32 * rows_f32, axis=-1, keepdims=True) + NORM_EPS)
    return (rows_f32 * inv_rms * gain_row.astype(jnp.float32)).astype(jnp.bfloat16)


def mat(rows_in, weight):
    return jnp.dot(rows_in, weight, preferred_element_type=jnp.float32)


def dense_kernel(finish_layer, local_layer, n_dev, *refs):
    refs = list(refs)
    take = lambda count: [refs.pop(0) for _ in range(count)]
    x_ref, ga_ref, gm_ref = take(3)
    o_ref = take(1)[0] if finish_layer is not None else None
    wq, wk, wv, wo, wg, wu, wd = take(7)
    kl_ref, vl_ref = take(2) if local_layer is not None else (None, None)
    y_ref = take(1)[0]
    outs = take(3) if local_layer is not None else []
    blocks, block_sem = take(2)
    width = x_ref.shape[1]
    n_ff = wg.shape[2] // width

    def mlp_blocks(layer):
        return [ref for part in range(n_ff) for ref in (wg.at[layer, :, pl.ds(part * width, width)], wu.at[layer, :, pl.ds(part * width, width)],
                                                        wd.at[layer, pl.ds(part * width, width), :])]

    sources = []
    if finish_layer is not None:
        sources += [wo.at[finish_layer]] + mlp_blocks(finish_layer)
    if local_layer is not None:
        sources += [w.at[local_layer] for w in (wk, wv, wq, wo)] + mlp_blocks(local_layer)
        sources += [w.at[local_layer + 1] for w in (wq, wk, wv)]
    copies = [pltpu.make_async_copy(source, blocks.at[at], block_sem.at[at]) for at, source in enumerate(sources)]

    if local_layer is not None:
        x_send, x_halo, klt, vlt, local_sem, halo_send, halo_recv = take(7)
        me = lax.axis_index('ctx')
        barrier = pltpu.get_barrier_semaphore()
        after, before = (me + 1) % n_dev, (me + n_dev - 1) % n_dev
        for neighbour in (after, before):
            pl.semaphore_signal(barrier, inc=1, device_id={'ctx': neighbour}, device_id_type=MESH_ID)
        pair = local_layer // 2
        local_copies = [pltpu.make_async_copy(kl_ref.at[pair], klt, local_sem.at[0]), pltpu.make_async_copy(vl_ref.at[pair], vlt, local_sem.at[1])]
        halo_source = x_ref if finish_layer is None else x_send
        halo = pltpu.make_async_remote_copy(src_ref=halo_source, dst_ref=x_halo, send_sem=halo_send, recv_sem=halo_recv,
                                            device_id={'ctx': after}, device_id_type=MESH_ID)
        for copy in local_copies:
            copy.start()
    for copy in copies:
        copy.start()
    if local_layer is not None:
        pl.semaphore_wait(barrier, 2)
        if finish_layer is None:
            halo.start()

    used = [0]

    def block():
        at = used[0]
        used[0] += 1
        copies[at].wait()
        return blocks[at]

    def mlp(hidden, layer):
        normed = rms_rows(hidden, gm_ref[layer:layer + 1, :])
        total = hidden.astype(jnp.float32)
        down = None
        for part in range(n_ff):
            gate_pre = mat(normed, block())
            up_pre = mat(normed, block())
            act = (jax.nn.gelu(gate_pre, approximate=True) * up_pre).astype(jnp.bfloat16)
            term = mat(act, block())
            down = term if down is None else down + term
        return (total + down).astype(jnp.bfloat16)

    hidden = x_ref[...]
    if finish_layer is not None:
        attn = o_ref[...].T
        hidden = (hidden.astype(jnp.float32) + mat(attn, block())).astype(jnp.bfloat16)
        hidden = mlp(hidden, finish_layer)
    if local_layer is None:
        y_ref[...] = hidden
        return
    if finish_layer is not None:
        x_send[...] = hidden
        halo.start()

    gain = ga_ref[local_layer:local_layer + 1, :]
    normed = rms_rows(hidden, gain)
    key_block = block()
    own_k = mat(normed, key_block).astype(jnp.bfloat16)
    value_block = block()
    own_vt = mat(normed, value_block).astype(jnp.bfloat16).T
    own_qt = mat(normed, block()).astype(jnp.bfloat16).T
    for copy in local_copies:
        copy.wait()
    first = me == 0
    n_rows = hidden.shape[0]
    heads, head_dim = kl_ref.shape[1], kl_ref.shape[2]
    halo.wait_recv()
    halo_normed = rms_rows(x_halo[...], gain)
    halo_k = mat(halo_normed, key_block).astype(jnp.bfloat16)
    halo_vt = mat(halo_normed, value_block).astype(jnp.bfloat16).T
    halo_k = jnp.where(first, klt[...].reshape(width, n_rows).T, halo_k)
    halo_vt = jnp.where(first, vlt[...].reshape(width, n_rows), halo_vt)
    keys = jnp.concatenate([halo_k, own_k], axis=0)
    values = jnp.concatenate([halo_vt, own_vt], axis=1)
    ahead = lax.broadcasted_iota(jnp.int32, (2 * n_rows, n_rows), 0) - lax.broadcasted_iota(jnp.int32, (2 * n_rows, n_rows), 1)
    seen = (ahead > 0) & (ahead <= n_rows)
    row = lax.broadcasted_iota(jnp.int32, (2 * head_dim, n_rows), 0)
    attn_t = []
    for head in range(heads):
        lanes = slice(2 * head_dim * (head // 2), 2 * head_dim * (head // 2 + 1))
        columns = jnp.where(row // head_dim == head % 2, own_qt[lanes, :], 0.0).astype(jnp.bfloat16)
        block_scores = mat(keys[:, lanes], columns) * (LOG2E * head_dim ** -0.5)
        block_scores = jnp.where(seen, block_scores, NEG)
        probs = jnp.exp2(block_scores - jnp.max(block_scores, axis=0, keepdims=True))
        below = jnp.sum(probs, axis=0, keepdims=True)
        attn_t.append((mat(values[head * head_dim:(head + 1) * head_dim, :], probs.astype(jnp.bfloat16)) / below).astype(jnp.bfloat16))
    attn = jnp.concatenate(attn_t, axis=0).T
    hidden = (hidden.astype(jnp.float32) + mat(attn, block())).astype(jnp.bfloat16)
    hidden = mlp(hidden, local_layer)
    y_ref[...] = hidden
    normed = rms_rows(hidden, ga_ref[local_layer + 1:local_layer + 2, :])
    for out in outs:
        out[...] = mat(normed, block()).astype(jnp.bfloat16).T.reshape(out.shape)
    halo.wait_send()


def dense(finish_layer, local_layer, n_dev, x_rows, gains, attn_t, weights, local_t):
    n_rows, width = x_rows.shape
    n_ff = weights[4].shape[2] // width
    vmem = pl.BlockSpec(memory_space=pltpu.VMEM)
    hbm = pl.BlockSpec(memory_space=pl.ANY)
    bf16 = jnp.bfloat16
    n_blocks = (0 if finish_layer is None else 1 + 3 * n_ff) + (0 if local_layer is None else 7 + 3 * n_ff)
    args, in_specs = [x_rows, *gains], [vmem] * 3
    out_shape, out_specs = [jax.ShapeDtypeStruct(x_rows.shape, bf16)], [vmem]
    scratch = [pltpu.VMEM((n_blocks, width, width), bf16), pltpu.SemaphoreType.DMA((n_blocks,))]
    if finish_layer is not None:
        args.append(attn_t)
        in_specs.append(vmem)
    args += weights
    in_specs += [hbm] * len(weights)
    params = {}
    if local_layer is not None:
        args += local_t
        in_specs += [hbm] * 2
        _, heads, head_dim, window = local_t[0].shape
        out_shape += [jax.ShapeDtypeStruct((heads, head_dim, n_rows), bf16)] * 3
        out_specs += [vmem] * 3
        scratch += [pltpu.VMEM(x_rows.shape, bf16), pltpu.VMEM(x_rows.shape, bf16),
                    pltpu.VMEM((heads, head_dim, window), bf16), pltpu.VMEM((heads, head_dim, window), bf16),
                    pltpu.SemaphoreType.DMA((2,)), pltpu.SemaphoreType.DMA, pltpu.SemaphoreType.DMA]
        params = dict(collective_id=8 + local_layer, has_side_effects=True)
    return pl.pallas_call(
        functools.partial(dense_kernel, finish_layer, local_layer, n_dev),
        out_shape=tuple(out_shape), in_specs=in_specs, out_specs=tuple(out_specs), scratch_shapes=scratch,
        compiler_params=pltpu.CompilerParams(vmem_limit_bytes=60 * 2 ** 20, **params),
        name='dense_%s_%s' % (finish_layer, local_layer),
    )(*args)


def solution(mesh):
    ctx_size = mesh.shape['ctx']
    row_spec = P(('dp', 'ctx'), None)
    cache_spec = P(None, ('dp', 'ctx'), None, None)
    local_spec = P(None, 'dp', None, None)
    in_specs = (row_spec, P('dp'), cache_spec, cache_spec, local_spec, local_spec) + (P(),) * 9

    def device_step(x_rows, cache_len, k_cache, v_cache, k_local, v_local, g_attn, g_mlp, *weights):
        by_slot = lambda array: jnp.transpose(array, (0, 2, 3, 1))
        cache_t = [by_slot(k_cache), by_slot(v_cache)]
        local_t = [by_slot(k_local), by_slot(v_local)]
        gains = [g_attn, g_mlp]
        hidden, finish_layer, attn_t = x_rows, None, None
        for pair in range(k_cache.shape[0]):
            hidden, *qkv = dense(finish_layer, 2 * pair, ctx_size, hidden, gains, attn_t, weights, local_t)
            attn_t = global_attention(pair, ctx_size, cache_len, *qkv, *cache_t)
            attn_t = attn_t.reshape(-1, attn_t.shape[-1])
            finish_layer = 2 * pair + 1
        return dense(finish_layer, None, ctx_size, hidden, gains, attn_t, weights, local_t)[0]

    return jax.shard_map(device_step, mesh=mesh, in_specs=in_specs, out_specs=row_spec, check_vma=False)
```

```python
import functools

import jax
import jax.numpy as jnp
from jax import lax
from jax.experimental import pallas as pl
from jax.experimental.pallas import tpu as pltpu
from jax.sharding import PartitionSpec as P

NORM_EPS = 1e-6
WINDOW = 4
LOG2E = 1.4426950408889634
NEG = -1e38
MESH_ID = pl.DeviceIdType.MESH
ROWS = 256
CHUNK = 256
STATS = 8


def slot_of(step):
    unit = step // 2
    return unit + unit // 2 - 2 * (unit // 3), step % 2


def global_kernel(n_chips, pair, len_ref, qkv_ref, kc_ref, vc_ref, out_ref,
                  k_own, v_own, k_sib, v_sib, kn_sib, vn_sib, q_all, k_ext, scores, part, parts,
                  own_sem, sib_send, sib_recv, q_send, q_recv, o_send, o_recv):
    q_ref, k_ref, v_ref = qkv_ref.at[0], qkv_ref.at[1], qkv_ref.at[2]
    heads, head_dim, slots = k_own.shape
    n_slots = 2 * n_chips
    me = lax.axis_index('ctx')
    chip, core = me // 2, me % 2
    first_head = heads * core
    other_head = heads * (1 - core)
    sibling = {'ctx': 2 * chip + (1 - core)}
    n_new = 2 * ROWS
    n_keys = 2 * slots + n_new

    barrier = pltpu.get_barrier_semaphore()
    for step in range(1, n_slots):
        pl.semaphore_signal(barrier, inc=1, device_id={'ctx': (me + step) % n_slots}, device_id_type=MESH_ID)

    def own_copies(head):
        return (pltpu.make_async_copy(kc_ref.at[pair, first_head + head], k_own.at[head], own_sem.at[0, head]),
                pltpu.make_async_copy(vc_ref.at[pair, first_head + head], v_own.at[head], own_sem.at[1, head]))

    def sib_copies(head):
        pairs = ((kc_ref.at[pair, other_head + head], k_sib.at[head]),
                 (vc_ref.at[pair, other_head + head], v_sib.at[head]),
                 (k_ref.at[other_head + head], kn_sib.at[head]),
                 (v_ref.at[other_head + head], vn_sib.at[head]))
        return [pltpu.make_async_remote_copy(src_ref=src, dst_ref=dst, send_sem=sib_send.at[which, head],
                                             recv_sem=sib_recv.at[which, head], device_id=sibling, device_id_type=MESH_ID)
                for which, (src, dst) in enumerate(pairs)]

    def target(dist, flip):
        return {'ctx': 2 * ((chip + dist) % n_chips) + (core + flip) % 2}

    def q_copy(dist, flip, head):
        slot = 2 * dist + flip
        their_head = heads * ((core + flip) % 2) + head
        return pltpu.make_async_remote_copy(src_ref=q_ref.at[their_head], dst_ref=q_all.at[slot, head],
                                            send_sem=q_send.at[slot, head], recv_sem=q_recv.at[slot, head],
                                            device_id=target(dist, flip), device_id_type=MESH_ID)

    def o_copy(dist, flip, head):
        slot = 2 * dist + flip
        owner = {'ctx': 2 * ((chip + n_chips - dist) % n_chips) + (core + flip) % 2}
        return pltpu.make_async_remote_copy(src_ref=part.at[slot, head], dst_ref=parts.at[slot, head],
                                            send_sem=o_send.at[slot, head], recv_sem=o_recv.at[slot, head],
                                            device_id=owner, device_id_type=MESH_ID)

    def start_own(head, carry):
        for copy in own_copies(head):
            copy.start()
        q_all[0, head] = q_ref[first_head + head]
        return carry

    lax.fori_loop(0, heads, start_own, 0)
    pl.semaphore_wait(barrier, n_slots - 1)

    def start_head(head, carry):
        for copy in sib_copies(head):
            copy.start()

        def start_q(step, inner):
            dist, flip = slot_of(step)
            q_copy(dist, flip, head).start()
            return inner

        lax.fori_loop(1, n_slots, start_q, 0)
        return carry

    lax.fori_loop(0, heads, start_head, 0)

    valid = len_ref[0]

    def prepare(head):
        for copy in own_copies(head):
            copy.wait()
        for copy in sib_copies(head):
            copy.wait_recv()
        width = 512
        row = lax.broadcasted_iota(jnp.int32, (head_dim, width), 0)
        col = lax.broadcasted_iota(jnp.int32, (head_dim, width), 1)
        for begin in range(0, n_keys, width):
            if begin < 2 * slots:
                source = k_own if begin < slots else k_sib
                at = begin % slots
                tile = source[head, :, at:at + width]
                device = me if begin < slots else 2 * chip + (1 - core)
                bias = jnp.where((row == 0) & (device * slots + at + col >= valid), NEG, 0.0)
            else:
                tile = jnp.concatenate([k_ref[first_head + head], kn_sib[head]], axis=1)
                bias = jnp.where((row == 1) & (col < ROWS) | (row == 2) & (col >= ROWS), 1.0, 0.0)
            buf = head % 2
            k_ext[buf, begin:begin + width, 0:2 * head_dim] = jnp.concatenate([tile, tile], axis=0).T
            k_ext[buf, begin:begin + width, 2 * head_dim:] = jnp.concatenate([tile, bias.astype(jnp.bfloat16)], axis=0).T

    def query_columns(head, dist, flip):
        slot = 2 * dist + flip
        full = q_all[slot, head].astype(jnp.float32) * (LOG2E * head_dim ** -0.5)
        high = full.astype(jnp.bfloat16)
        rest = full - high.astype(jnp.float32)
        middle = rest.astype(jnp.bfloat16)
        low = (rest - middle.astype(jnp.float32)).astype(jnp.bfloat16)
        q_dev = 2 * ((chip + n_chips - dist) % n_chips) + (core + flip) % 2
        row = lax.broadcasted_iota(jnp.int32, (head_dim, ROWS), 0)
        hide_own = jnp.where(q_dev < me, NEG, 0.0)
        hide_sib = jnp.where(q_dev < 2 * chip + (1 - core), NEG, 0.0)
        mask = jnp.where(row == 0, 1.0, jnp.where(row == 1, hide_own, jnp.where(row == 2, hide_sib, 0.0)))
        return jnp.concatenate([high, middle, low, mask.astype(jnp.bfloat16)], axis=0), q_dev

    def score_chunk(buf, columns, q_dev, begin, top):
        keys = pl.ds(begin, CHUNK)
        block = jnp.dot(k_ext[buf, keys, :], columns, preferred_element_type=jnp.float32)
        if begin >= 2 * slots:
            device = me if begin < 2 * slots + ROWS else 2 * chip + (1 - core)
            ahead = lax.broadcasted_iota(jnp.int32, (CHUNK, ROWS), 0) - lax.broadcasted_iota(jnp.int32, (CHUNK, ROWS), 1)
            block = jnp.where(ahead <= jnp.where(q_dev == device, 0, ROWS), block, NEG)
        scores[keys, :] = block
        return jnp.maximum(top, jnp.max(block.reshape(CHUNK // 8, 8, ROWS), axis=0))

    def value_chunk(head, base, begin, total, weighted):
        keys = pl.ds(begin, CHUNK)
        probs = jnp.exp2(scores[keys, :] - base)
        total = total + jnp.sum(probs.reshape(CHUNK // 8, 8, ROWS), axis=0)
        if begin < slots:
            values = v_own[head, :, begin:begin + CHUNK]
        elif begin < 2 * slots:
            values = v_sib[head, :, begin - slots:begin - slots + CHUNK]
        elif begin < 2 * slots + ROWS:
            values = v_ref[first_head + head]
        else:
            values = vn_sib[head]
        return total, weighted + jnp.dot(values, probs.astype(jnp.bfloat16), preferred_element_type=jnp.float32)

    no_top = jnp.full((8, ROWS), NEG, jnp.float32)

    prepare(0)
    columns, q_dev = query_columns(0, 0, 0)
    top = no_top
    for begin in range(0, n_keys, CHUNK):
        top = score_chunk(0, columns, q_dev, begin, top)

    def one_head(head, top):
        next_head = jnp.minimum(head + 1, heads - 1)

        @pl.when(head < heads - 1)
        def _():
            prepare(next_head)

        def one_step(step, top):
            dist, flip = slot_of(step)
            slot = 2 * dist + flip
            after = (step + 1) % n_slots
            dist_n, flip_n = slot_of(after)
            head_n = jnp.where(step == n_slots - 1, next_head, head)

            @pl.when(after > 0)
            def _():
                q_copy(dist_n, flip_n, head).wait_recv()

            columns, q_dev = query_columns(head_n, dist_n, flip_n)
            base = jnp.max(top, axis=0, keepdims=True)
            total = jnp.zeros((8, ROWS), jnp.float32)
            weighted = jnp.zeros((head_dim, ROWS), jnp.float32)
            new_top = no_top
            for begin in range(0, n_keys, CHUNK):
                total, weighted = value_chunk(head, base, begin, total, weighted)
                new_top = score_chunk(head_n % 2, columns, q_dev, begin, new_top)
            row = lax.broadcasted_iota(jnp.int32, (STATS, ROWS), 0)
            total = jnp.sum(total, axis=0, keepdims=True)
            part[slot, head, 0:head_dim, :] = weighted
            part[slot, head, head_dim:, :] = jnp.where(row == 0, base, total)

            @pl.when(step > 0)
            def _():
                o_copy(dist, flip, head).start()

            return new_top

        return lax.fori_loop(0, n_slots, one_step, top)

    lax.fori_loop(0, heads, one_head, top)

    def merge(head, carry):
        for flip in range(2):
            found = []
            for dist in range(n_chips):
                slot = 2 * dist + flip
                if slot == 0:
                    found.append((part[0, head, 0:head_dim, :], part[0, head, head_dim:head_dim + 1, :],
                                  part[0, head, head_dim + 1:head_dim + 2, :]))
                else:
                    o_copy(dist, flip, head).wait_recv()
                    found.append((parts[slot, head, 0:head_dim, :], parts[slot, head, head_dim:head_dim + 1, :],
                                  parts[slot, head, head_dim + 1:head_dim + 2, :]))
            peak = functools.reduce(jnp.maximum, [base for _, base, _ in found])
            scaled = [(weighted, total, jnp.exp2(base - peak)) for weighted, base, total in found]
            upper = sum(weighted * factor for weighted, _, factor in scaled)
            lower = sum(total * factor for _, total, factor in scaled)
            out_ref[heads * ((core + flip) % 2) + head] = (upper / lower).astype(jnp.bfloat16)
        return carry

    lax.fori_loop(0, heads, merge, 0)

    def finish(head, carry):
        for copy in sib_copies(head):
            copy.wait_send()

        def finish_step(step, inner):
            dist, flip = slot_of(step)
            q_copy(dist, flip, head).wait_send()
            o_copy(dist, flip, head).wait_send()
            return inner

        lax.fori_loop(1, n_slots, finish_step, 0)
        return carry

    lax.fori_loop(0, heads, finish, 0)


def global_attention(pair, n_dev, valid_len, qkv, cache_k, cache_v):
    _, all_heads, head_dim, rows = qkv.shape
    heads = all_heads // 2
    slots = cache_k.shape[-1]
    n_keys = 2 * (slots + rows)
    vmem = pl.BlockSpec(memory_space=pltpu.VMEM)
    bf16, f32 = jnp.bfloat16, jnp.float32
    return pl.pallas_call(
        functools.partial(global_kernel, n_dev // 2, pair),
        out_shape=jax.ShapeDtypeStruct((all_heads, head_dim, rows), bf16),
        in_specs=[pl.BlockSpec(memory_space=pltpu.SMEM), vmem,
                  pl.BlockSpec(memory_space=pl.ANY), pl.BlockSpec(memory_space=pl.ANY)],
        out_specs=vmem,
        scratch_shapes=[
            pltpu.VMEM((heads, head_dim, slots), bf16), pltpu.VMEM((heads, head_dim, slots), bf16),
            pltpu.VMEM((heads, head_dim, slots), bf16), pltpu.VMEM((heads, head_dim, slots), bf16),
            pltpu.VMEM((heads, head_dim, rows), bf16), pltpu.VMEM((heads, head_dim, rows), bf16),
            pltpu.VMEM((n_dev, heads, head_dim, rows), bf16),
            pltpu.VMEM((2, n_keys, 4 * head_dim), bf16),
            pltpu.VMEM((n_keys, rows), f32),
            pltpu.VMEM((n_dev, heads, head_dim + STATS, rows), f32),
            pltpu.VMEM((n_dev, heads, head_dim + STATS, rows), f32),
            pltpu.SemaphoreType.DMA((2, heads)),
            pltpu.SemaphoreType.DMA((4, heads)), pltpu.SemaphoreType.DMA((4, heads)),
            pltpu.SemaphoreType.DMA((n_dev, heads)), pltpu.SemaphoreType.DMA((n_dev, heads)),
            pltpu.SemaphoreType.DMA((n_dev, heads)), pltpu.SemaphoreType.DMA((n_dev, heads)),
        ],
        compiler_params=pltpu.CompilerParams(collective_id=pair, has_side_effects=True, vmem_limit_bytes=56 * 2 ** 20),
        name='global_attn_%d' % pair,
    )(valid_len, qkv, cache_k, cache_v)


def rms_rows(rows_in, gain_row):
    rows_f32 = rows_in.astype(jnp.float32)
    inv_rms = lax.rsqrt(jnp.mean(rows_f32 * rows_f32, axis=-1, keepdims=True) + NORM_EPS)
    return (rows_f32 * inv_rms * gain_row.astype(jnp.float32)).astype(jnp.bfloat16)


def mat(rows_in, weight):
    return jnp.dot(rows_in, weight, preferred_element_type=jnp.float32)


def dense_kernel(finish_layer, local_layer, n_dev, *refs):
    refs = list(refs)
    take = lambda count: [refs.pop(0) for _ in range(count)]
    x_ref, ga_ref, gm_ref = take(3)
    o_ref = take(1)[0] if finish_layer is not None else None
    wq, wk, wv, wo, wg, wu, wd = take(7)
    kl_ref, vl_ref = take(2) if local_layer is not None else (None, None)
    y_ref = take(1)[0]
    qkv_ref = take(1)[0] if local_layer is not None else None
    blocks, block_sem, rows_ref, acts, sums = take(5)
    n_rows, width = x_ref.shape
    n_ff = wg.shape[2] // width

    def weight_copy(source, at):
        return pltpu.make_async_copy(source, blocks.at[at], block_sem.at[at])

    def ff_copies(layer, base, part):
        span = pl.ds(pl.multiple_of(part * width, width), width)
        return [weight_copy(source, base + 3 * part + which)
                for which, source in enumerate((wg.at[layer, :, span], wu.at[layer, :, span], wd.at[layer, span, :]))]

    finish_base = 1
    local_base = (0 if finish_layer is None else 1 + 3 * n_ff) + 4
    next_base = local_base + 3 * n_ff
    plan = []
    if finish_layer is not None:
        plan += [weight_copy(wo.at[finish_layer], 0)]
        plan += [copy for part in range(n_ff) for copy in ff_copies(finish_layer, finish_base, part)]
    if local_layer is not None:
        plan += [weight_copy(w.at[local_layer], local_base - 4 + which) for which, w in enumerate((wk, wv, wq, wo))]
        plan += [copy for part in range(n_ff) for copy in ff_copies(local_layer, local_base, part)]
        plan += [weight_copy(w.at[local_layer + 1], next_base + which) for which, w in enumerate((wq, wk, wv))]
    started = [0]

    def fetch(limit):
        for copy in plan[started[0]:limit]:
            copy.start()
        started[0] = max(started[0], min(limit, len(plan)))

    fetch(WINDOW)
    if local_layer is not None:
        x_send, x_halo, klt, vlt, keys, values, queries, attn_t, local_sem, halo_send, halo_recv = take(11)
        me = lax.axis_index('ctx')
        barrier = pltpu.get_barrier_semaphore()
        after, before = (me + 1) % n_dev, (me + n_dev - 1) % n_dev
        for neighbour in (after, before):
            pl.semaphore_signal(barrier, inc=1, device_id={'ctx': neighbour}, device_id_type=MESH_ID)
        pair = local_layer // 2
        local_copies = [pltpu.make_async_copy(kl_ref.at[pair], klt, local_sem.at[0]), pltpu.make_async_copy(vl_ref.at[pair], vlt, local_sem.at[1])]
        halo = pltpu.make_async_remote_copy(src_ref=x_ref if finish_layer is None else x_send, dst_ref=x_halo, send_sem=halo_send,
                                            recv_sem=halo_recv, device_id={'ctx': after}, device_id_type=MESH_ID)
        for copy in local_copies:
            copy.start()
        if finish_layer is None:
            pl.semaphore_wait(barrier, 2)
            halo.start()

    def block(at):
        fetch(at + WINDOW)
        plan[at].wait()
        return blocks[at]

    def mlp(hidden, layer, base):
        fetch(base + 3 * n_ff)
        rows_ref[...] = rms_rows(hidden, gm_ref[layer:layer + 1, :])
        sums[...] = hidden.astype(jnp.float32)

        def activate(part):
            gate_pre = mat(rows_ref[...], blocks[base + 3 * part])
            up_pre = mat(rows_ref[...], blocks[base + 3 * part + 1])
            acts[part % 2] = (jax.nn.gelu(gate_pre, approximate=True) * up_pre).astype(jnp.bfloat16)

        def shrink(part):
            sums[...] += mat(acts[part % 2], blocks[base + 3 * part + 2])

        def arrive(part):
            for copy in ff_copies(layer, base, part):
                copy.wait()

        arrive(0)
        activate(0)

        def step(part, carry):
            arrive(part)
            shrink(part - 1)
            activate(part)
            return carry

        lax.fori_loop(1, n_ff, step, 0)
        fetch(base + 3 * n_ff + WINDOW)
        shrink(n_ff - 1)
        return sums[...].astype(jnp.bfloat16)

    hidden = x_ref[...]
    if finish_layer is not None:
        attn = o_ref[...].T
        hidden = (hidden.astype(jnp.float32) + mat(attn, block(0))).astype(jnp.bfloat16)
        hidden = mlp(hidden, finish_layer, finish_base)
    if local_layer is None:
        y_ref[...] = hidden
        return
    if finish_layer is not None:
        x_send[...] = hidden
        pl.semaphore_wait(barrier, 2)
        halo.start()

    heads, head_dim = kl_ref.shape[1], kl_ref.shape[2]
    at = local_base - 4
    gain = ga_ref[local_layer:local_layer + 1, :]
    rows_ref[...] = rms_rows(hidden, gain)
    key_block = block(at)
    keys[n_rows:, :] = mat(rows_ref[...], key_block).astype(jnp.bfloat16)
    value_block = block(at + 1)
    values[:, n_rows:] = mat(rows_ref[...], value_block).astype(jnp.bfloat16).T
    queries[...] = mat(rows_ref[...], block(at + 2)).astype(jnp.bfloat16).T
    for copy in local_copies:
        copy.wait()
    fetch(at + 4 + WINDOW)
    first = me == 0
    halo.wait_recv()
    rows_ref[...] = rms_rows(x_halo[...], gain)
    keys[:n_rows, :] = jnp.where(first, klt[...].reshape(width, n_rows).T, mat(rows_ref[...], blocks[at]).astype(jnp.bfloat16))
    values[:, :n_rows] = jnp.where(first, vlt[...].reshape(width, n_rows), mat(rows_ref[...], blocks[at + 1]).astype(jnp.bfloat16).T)
    ahead = lax.broadcasted_iota(jnp.int32, (2 * n_rows, n_rows), 0) - lax.broadcasted_iota(jnp.int32, (2 * n_rows, n_rows), 1)
    seen = (ahead > 0) & (ahead <= n_rows)
    row = lax.broadcasted_iota(jnp.int32, (2 * head_dim, n_rows), 0)

    def head_pair(pair_at, carry):
        lanes = pl.ds(pl.multiple_of(2 * head_dim * pair_at, 2 * head_dim), 2 * head_dim)
        for half in range(2):
            columns = jnp.where(row // head_dim == half, queries[lanes, :], 0.0).astype(jnp.bfloat16)
            block_scores = mat(keys[:, lanes], columns) * (LOG2E * head_dim ** -0.5)
            block_scores = jnp.where(seen, block_scores, NEG)
            probs = jnp.exp2(block_scores - jnp.max(block_scores, axis=0, keepdims=True))
            below = jnp.sum(probs, axis=0, keepdims=True)
            rows = pl.ds(pl.multiple_of(2 * head_dim * pair_at + half * head_dim, head_dim), head_dim)
            attn_t[rows, :] = (mat(values[rows, :], probs.astype(jnp.bfloat16)) / below).astype(jnp.bfloat16)
        return carry

    lax.fori_loop(0, heads // 2, head_pair, 0)
    hidden = (hidden.astype(jnp.float32) + mat(attn_t[...].T, block(at + 3))).astype(jnp.bfloat16)
    hidden = mlp(hidden, local_layer, local_base)
    y_ref[...] = hidden
    rows_ref[...] = rms_rows(hidden, ga_ref[local_layer + 1:local_layer + 2, :])
    fetch(len(plan))

    def project(which, carry):
        weight_copy(wq.at[local_layer + 1], next_base + which).wait()
        qkv_ref[which] = mat(rows_ref[...], blocks[next_base + which]).astype(jnp.bfloat16).T.reshape(qkv_ref.shape[1:])
        return carry

    lax.fori_loop(0, 3, project, 0)
    halo.wait_send()


def dense(finish_layer, local_layer, n_dev, x_rows, gains, attn_t, weights, local_t):
    n_rows, width = x_rows.shape
    n_ff = weights[4].shape[2] // width
    vmem = pl.BlockSpec(memory_space=pltpu.VMEM)
    hbm = pl.BlockSpec(memory_space=pl.ANY)
    bf16 = jnp.bfloat16
    n_blocks = (0 if finish_layer is None else 1 + 3 * n_ff) + (0 if local_layer is None else 7 + 3 * n_ff)
    args, in_specs = [x_rows, *gains], [vmem] * 3
    out_shape, out_specs = [jax.ShapeDtypeStruct(x_rows.shape, bf16)], [vmem]
    scratch = [pltpu.VMEM((n_blocks, width, width), bf16), pltpu.SemaphoreType.DMA((n_blocks,)),
               pltpu.VMEM(x_rows.shape, bf16), pltpu.VMEM((2, *x_rows.shape), bf16), pltpu.VMEM(x_rows.shape, jnp.float32)]
    if finish_layer is not None:
        args.append(attn_t)
        in_specs.append(vmem)
    args += weights
    in_specs += [hbm] * len(weights)
    params = {}
    if local_layer is not None:
        args += local_t
        in_specs += [hbm] * 2
        _, heads, head_dim, window = local_t[0].shape
        out_shape += [jax.ShapeDtypeStruct((3, heads, head_dim, n_rows), bf16)]
        out_specs += [vmem]
        scratch += [pltpu.VMEM(x_rows.shape, bf16), pltpu.VMEM(x_rows.shape, bf16),
                    pltpu.VMEM((heads, head_dim, window), bf16), pltpu.VMEM((heads, head_dim, window), bf16),
                    pltpu.VMEM((window + n_rows, width), bf16), pltpu.VMEM((width, window + n_rows), bf16),
                    pltpu.VMEM((width, n_rows), bf16), pltpu.VMEM((width, n_rows), bf16),
                    pltpu.SemaphoreType.DMA((2,)), pltpu.SemaphoreType.DMA, pltpu.SemaphoreType.DMA]
        params = dict(collective_id=8 + local_layer, has_side_effects=True)
    return pl.pallas_call(
        functools.partial(dense_kernel, finish_layer, local_layer, n_dev),
        out_shape=tuple(out_shape), in_specs=in_specs, out_specs=tuple(out_specs), scratch_shapes=scratch,
        compiler_params=pltpu.CompilerParams(vmem_limit_bytes=60 * 2 ** 20, **params),
        name='dense_%s_%s' % (finish_layer, local_layer),
    )(*args)


def solution(mesh):
    ctx_size = mesh.shape['ctx']
    row_spec = P(('dp', 'ctx'), None)
    cache_spec = P(None, ('dp', 'ctx'), None, None)
    local_spec = P(None, 'dp', None, None)
    in_specs = (row_spec, P('dp'), cache_spec, cache_spec, local_spec, local_spec) + (P(),) * 9

    def device_step(x_rows, cache_len, k_cache, v_cache, k_local, v_local, g_attn, g_mlp, *weights):
        by_slot = lambda array: jnp.transpose(array, (0, 2, 3, 1))
        cache_t = [by_slot(k_cache), by_slot(v_cache)]
        local_t = [by_slot(k_local), by_slot(v_local)]
        gains = [g_attn, g_mlp]
        hidden, finish_layer, attn_t = x_rows, None, None
        for pair in range(k_cache.shape[0]):
            hidden, qkv = dense(finish_layer, 2 * pair, ctx_size, hidden, gains, attn_t, weights, local_t)
            attn_t = global_attention(pair, ctx_size, cache_len, qkv, *cache_t)
            attn_t = attn_t.reshape(-1, attn_t.shape[-1])
            finish_layer = 2 * pair + 1
        return dense(finish_layer, None, ctx_size, hidden, gains, attn_t, weights, local_t)[0]

    return jax.shard_map(device_step, mesh=mesh, in_specs=in_specs, out_specs=row_spec, check_vma=False)
```

```python
import functools

import jax
import jax.numpy as jnp
from jax import lax
from jax.experimental import pallas as pl
from jax.experimental.pallas import tpu as pltpu
from jax.sharding import PartitionSpec as P

NORM_EPS = 1e-6
WINDOW = 4
LOG2E = 1.4426950408889634
NEG = -1e38
MESH_ID = pl.DeviceIdType.MESH
ROWS = 256
SCORE_KEYS = 1152
VALUE_KEYS = 128
STATS = 8


def slot_of(step, head, n_slots):
    place = jnp.where(head == 0, step, n_slots - 1 - step)
    unit = place // 2
    return unit + unit // 2 - 2 * (unit // 3), place % 2


def global_kernel(n_chips, pair, len_ref, qkv_ref, kc_ref, vc_ref, out_ref,
                  k_own, v_own, k_sib, v_sib, kn_sib, vn_sib, q_all, k_twice, k_mask, scores, part, parts,
                  own_sem, sib_send, sib_recv, q_send, q_recv, o_send, o_recv):
    q_ref, k_ref, v_ref = qkv_ref.at[0], qkv_ref.at[1], qkv_ref.at[2]
    heads, head_dim, slots = k_own.shape
    n_slots = 2 * n_chips
    me = lax.axis_index('ctx')
    chip, core = me // 2, me % 2
    first_head = heads * core
    other_head = heads * (1 - core)
    sibling = {'ctx': 2 * chip + (1 - core)}
    n_new = 2 * ROWS
    n_keys = 2 * slots + n_new

    barrier = pltpu.get_barrier_semaphore()
    for step in range(1, n_slots):
        pl.semaphore_signal(barrier, inc=1, device_id={'ctx': (me + step) % n_slots}, device_id_type=MESH_ID)

    def own_copies(head):
        return (pltpu.make_async_copy(kc_ref.at[pair, first_head + head], k_own.at[head], own_sem.at[0, head]),
                pltpu.make_async_copy(vc_ref.at[pair, first_head + head], v_own.at[head], own_sem.at[1, head]))

    def sib_copies(head):
        pairs = ((kc_ref.at[pair, other_head + head], k_sib.at[head]),
                 (vc_ref.at[pair, other_head + head], v_sib.at[head]),
                 (k_ref.at[other_head + head], kn_sib.at[head]),
                 (v_ref.at[other_head + head], vn_sib.at[head]))
        return [pltpu.make_async_remote_copy(src_ref=src, dst_ref=dst, send_sem=sib_send.at[which, head],
                                             recv_sem=sib_recv.at[which, head], device_id=sibling, device_id_type=MESH_ID)
                for which, (src, dst) in enumerate(pairs)]

    def target(dist, flip):
        return {'ctx': 2 * ((chip + dist) % n_chips) + (core + flip) % 2}

    def q_copy(dist, flip, head):
        slot = 2 * dist + flip
        their_head = heads * ((core + flip) % 2) + head
        return pltpu.make_async_remote_copy(src_ref=q_ref.at[their_head], dst_ref=q_all.at[slot, head],
                                            send_sem=q_send.at[slot, head], recv_sem=q_recv.at[slot, head],
                                            device_id=target(dist, flip), device_id_type=MESH_ID)

    def o_copy(dist, flip, head):
        slot = 2 * dist + flip
        owner = {'ctx': 2 * ((chip + n_chips - dist) % n_chips) + (core + flip) % 2}
        return pltpu.make_async_remote_copy(src_ref=part.at[slot, head], dst_ref=parts.at[slot, head],
                                            send_sem=o_send.at[slot, head], recv_sem=o_recv.at[slot, head],
                                            device_id=owner, device_id_type=MESH_ID)

    def start_own(head, carry):
        for copy in own_copies(head):
            copy.start()
        q_all[0, head] = q_ref[first_head + head]
        return carry

    lax.fori_loop(0, heads, start_own, 0)
    pl.semaphore_wait(barrier, n_slots - 1)

    def start_head(head, carry):
        for copy in sib_copies(head):
            copy.start()

        def start_q(step, inner):
            dist, flip = slot_of(step, 0, n_slots)
            q_copy(dist, flip, head).start()
            return inner

        lax.fori_loop(1, n_slots, start_q, 0)
        return carry

    lax.fori_loop(0, heads, start_head, 0)

    valid = len_ref[0]

    def prepare(head):
        for copy in own_copies(head):
            copy.wait()
        for copy in sib_copies(head):
            copy.wait_recv()
        width = 512
        row = lax.broadcasted_iota(jnp.int32, (head_dim, width), 0)
        col = lax.broadcasted_iota(jnp.int32, (head_dim, width), 1)
        for begin in range(0, n_keys, width):
            if begin < 2 * slots:
                source = k_own if begin < slots else k_sib
                at = begin % slots
                tile = source[head, :, at:at + width]
                device = me if begin < slots else 2 * chip + (1 - core)
                bias = jnp.where((row == 0) & (device * slots + at + col >= valid), NEG, 0.0)
            else:
                tile = jnp.concatenate([k_ref[first_head + head], kn_sib[head]], axis=1)
                bias = jnp.where((row == 1) & (col < ROWS) | (row == 2) & (col >= ROWS), 1.0, 0.0)
            buf = head % 2
            k_twice[buf, begin:begin + width, :] = jnp.concatenate([tile, tile], axis=0).T
            k_mask[buf, begin:begin + width, :] = jnp.concatenate([tile, bias.astype(jnp.bfloat16)], axis=0).T

    def query_columns(head, dist, flip):
        slot = 2 * dist + flip
        full = q_all[slot, head].astype(jnp.float32) * (LOG2E * head_dim ** -0.5)
        high = full.astype(jnp.bfloat16)
        rest = full - high.astype(jnp.float32)
        middle = rest.astype(jnp.bfloat16)
        low = (rest - middle.astype(jnp.float32)).astype(jnp.bfloat16)
        q_dev = 2 * ((chip + n_chips - dist) % n_chips) + (core + flip) % 2
        row = lax.broadcasted_iota(jnp.int32, (head_dim, ROWS), 0)
        hide_own = jnp.where(q_dev < me, NEG, 0.0)
        hide_sib = jnp.where(q_dev < 2 * chip + (1 - core), NEG, 0.0)
        mask = jnp.where(row == 0, 1.0, jnp.where(row == 1, hide_own, jnp.where(row == 2, hide_sib, 0.0)))
        return jnp.concatenate([high, middle, low, mask.astype(jnp.bfloat16)], axis=0), q_dev

    def score_chunk(buf, columns, q_dev, begin, top):
        keys = pl.ds(begin, SCORE_KEYS)
        rows = jnp.concatenate([k_twice[buf, keys, :], k_mask[buf, keys, :]], axis=1)
        block = jnp.dot(rows, columns, preferred_element_type=jnp.float32)
        plain = min(max(2 * slots - begin, 0), SCORE_KEYS)
        pieces = [block[:plain]] if plain else []
        for at in range(plain, SCORE_KEYS, ROWS):
            device = me if begin + at < 2 * slots + ROWS else 2 * chip + (1 - core)
            ahead = lax.broadcasted_iota(jnp.int32, (ROWS, ROWS), 0) - lax.broadcasted_iota(jnp.int32, (ROWS, ROWS), 1)
            pieces.append(jnp.where(ahead <= jnp.where(q_dev == device, 0, ROWS), block[at:at + ROWS], NEG))
        at = begin
        for piece in pieces:
            scores[pl.ds(at, piece.shape[0]), :] = piece
            top = jnp.maximum(top, jnp.max(piece.reshape(piece.shape[0] // 8, 8, ROWS), axis=0))
            at += piece.shape[0]
        return top

    def value_chunk(head, base, begin, total, weighted):
        probs = jnp.exp2(scores[pl.ds(begin, VALUE_KEYS), :] - base)
        total = total + jnp.sum(probs.reshape(VALUE_KEYS // 8, 8, ROWS), axis=0)
        if begin < slots:
            values = v_own[head, :, begin:begin + VALUE_KEYS]
        elif begin < 2 * slots:
            values = v_sib[head, :, begin - slots:begin - slots + VALUE_KEYS]
        elif begin < 2 * slots + ROWS:
            values = v_ref[first_head + head, :, begin - 2 * slots:begin - 2 * slots + VALUE_KEYS]
        else:
            values = vn_sib[head, :, begin - 2 * slots - ROWS:begin - 2 * slots - ROWS + VALUE_KEYS]
        return total, weighted + jnp.dot(values, probs.astype(jnp.bfloat16), preferred_element_type=jnp.float32)

    order = sorted([(begin + VALUE_KEYS, 0, begin) for begin in range(0, n_keys, VALUE_KEYS)]
                   + [(begin + SCORE_KEYS, 1, begin) for begin in range(0, n_keys, SCORE_KEYS)])
    no_top = jnp.full((8, ROWS), NEG, jnp.float32)

    prepare(0)
    columns, q_dev = query_columns(0, 0, 0)
    top = no_top
    for begin in range(0, n_keys, SCORE_KEYS):
        top = score_chunk(0, columns, q_dev, begin, top)

    def one_head(head, top):
        next_head = jnp.minimum(head + 1, heads - 1)

        @pl.when(head < heads - 1)
        def _():
            prepare(next_head)

        def one_step(step, top):
            dist, flip = slot_of(step, head, n_slots)
            slot = 2 * dist + flip
            after = (step + 1) % n_slots
            head_n = jnp.where(step == n_slots - 1, next_head, head)
            dist_n, flip_n = slot_of(after, head_n, n_slots)
            remote_n = (2 * dist_n + flip_n > 0) & ((step < n_slots - 1) | (head < heads - 1))

            @pl.when(remote_n)
            def _():
                q_copy(dist_n, flip_n, head_n).wait_recv()

            columns, q_dev = query_columns(head_n, dist_n, flip_n)
            base = jnp.max(top, axis=0, keepdims=True)
            total = jnp.zeros((8, ROWS), jnp.float32)
            weighted = jnp.zeros((head_dim, ROWS), jnp.float32)
            new_top = no_top
            for _, kind, begin in order:
                if kind == 0:
                    total, weighted = value_chunk(head, base, begin, total, weighted)
                else:
                    new_top = score_chunk(head_n % 2, columns, q_dev, begin, new_top)
            row = lax.broadcasted_iota(jnp.int32, (STATS, ROWS), 0)
            total = jnp.sum(total, axis=0, keepdims=True)
            part[slot, head, 0:head_dim, :] = weighted
            part[slot, head, head_dim:, :] = jnp.where(row == 0, base, total)

            @pl.when(slot > 0)
            def _():
                o_copy(dist, flip, head).start()

            return new_top

        return lax.fori_loop(0, n_slots, one_step, top)

    lax.fori_loop(0, heads, one_head, top)

    def merge(head, carry):
        for flip in range(2):
            found = []
            for dist in range(n_chips):
                slot = 2 * dist + flip
                if slot == 0:
                    found.append((part[0, head, 0:head_dim, :], part[0, head, head_dim:head_dim + 1, :],
                                  part[0, head, head_dim + 1:head_dim + 2, :]))
                else:
                    o_copy(dist, flip, head).wait_recv()
                    found.append((parts[slot, head, 0:head_dim, :], parts[slot, head, head_dim:head_dim + 1, :],
                                  parts[slot, head, head_dim + 1:head_dim + 2, :]))
            peak = functools.reduce(jnp.maximum, [base for _, base, _ in found])
            scaled = [(weighted, total, jnp.exp2(base - peak)) for weighted, base, total in found]
            upper = sum(weighted * factor for weighted, _, factor in scaled)
            lower = sum(total * factor for _, total, factor in scaled)
            out_ref[heads * ((core + flip) % 2) + head] = (upper / lower).astype(jnp.bfloat16)
        return carry

    lax.fori_loop(0, heads, merge, 0)

    def finish(head, carry):
        for copy in sib_copies(head):
            copy.wait_send()

        def finish_step(step, inner):
            dist, flip = slot_of(step, 0, n_slots)
            q_copy(dist, flip, head).wait_send()
            o_copy(dist, flip, head).wait_send()
            return inner

        lax.fori_loop(1, n_slots, finish_step, 0)
        return carry

    lax.fori_loop(0, heads, finish, 0)


def global_attention(pair, n_dev, valid_len, qkv, cache_k, cache_v):
    _, all_heads, head_dim, rows = qkv.shape
    heads = all_heads // 2
    slots = cache_k.shape[-1]
    n_keys = 2 * (slots + rows)
    vmem = pl.BlockSpec(memory_space=pltpu.VMEM)
    bf16, f32 = jnp.bfloat16, jnp.float32
    return pl.pallas_call(
        functools.partial(global_kernel, n_dev // 2, pair),
        out_shape=jax.ShapeDtypeStruct((all_heads, head_dim, rows), bf16),
        in_specs=[pl.BlockSpec(memory_space=pltpu.SMEM), vmem,
                  pl.BlockSpec(memory_space=pl.ANY), pl.BlockSpec(memory_space=pl.ANY)],
        out_specs=vmem,
        scratch_shapes=[
            pltpu.VMEM((heads, head_dim, slots), bf16), pltpu.VMEM((heads, head_dim, slots), bf16),
            pltpu.VMEM((heads, head_dim, slots), bf16), pltpu.VMEM((heads, head_dim, slots), bf16),
            pltpu.VMEM((heads, head_dim, rows), bf16), pltpu.VMEM((heads, head_dim, rows), bf16),
            pltpu.VMEM((n_dev, heads, head_dim, rows), bf16),
            pltpu.VMEM((2, n_keys, 2 * head_dim), bf16), pltpu.VMEM((2, n_keys, 2 * head_dim), bf16),
            pltpu.VMEM((n_keys, rows), f32),
            pltpu.VMEM((n_dev, heads, head_dim + STATS, rows), f32),
            pltpu.VMEM((n_dev, heads, head_dim + STATS, rows), f32),
            pltpu.SemaphoreType.DMA((2, heads)),
            pltpu.SemaphoreType.DMA((4, heads)), pltpu.SemaphoreType.DMA((4, heads)),
            pltpu.SemaphoreType.DMA((n_dev, heads)), pltpu.SemaphoreType.DMA((n_dev, heads)),
            pltpu.SemaphoreType.DMA((n_dev, heads)), pltpu.SemaphoreType.DMA((n_dev, heads)),
        ],
        compiler_params=pltpu.CompilerParams(collective_id=pair, has_side_effects=True, vmem_limit_bytes=56 * 2 ** 20),
        name='global_attn_%d' % pair,
    )(valid_len, qkv, cache_k, cache_v)


def rms_rows(rows_in, gain_row):
    rows_f32 = rows_in.astype(jnp.float32)
    inv_rms = lax.rsqrt(jnp.mean(rows_f32 * rows_f32, axis=-1, keepdims=True) + NORM_EPS)
    return (rows_f32 * inv_rms * gain_row.astype(jnp.float32)).astype(jnp.bfloat16)


def mat(rows_in, weight):
    return jnp.dot(rows_in, weight, preferred_element_type=jnp.float32)


def dense_kernel(finish_layer, local_layer, n_dev, *refs):
    refs = list(refs)
    take = lambda count: [refs.pop(0) for _ in range(count)]
    x_ref, ga_ref, gm_ref = take(3)
    o_ref = take(1)[0] if finish_layer is not None else None
    wq, wk, wv, wo, wg, wu, wd = take(7)
    kl_ref, vl_ref = take(2) if local_layer is not None else (None, None)
    y_ref = take(1)[0]
    qkv_ref = take(1)[0] if local_layer is not None else None
    blocks, block_sem, rows_ref, acts, sums = take(5)
    n_rows, width = x_ref.shape
    n_ff = wg.shape[2] // width

    def weight_copy(source, at):
        return pltpu.make_async_copy(source, blocks.at[at], block_sem.at[at])

    def ff_copies(layer, base, part):
        span = pl.ds(pl.multiple_of(part * width, width), width)
        return [weight_copy(source, base + 3 * part + which)
                for which, source in enumerate((wg.at[layer, :, span], wu.at[layer, :, span], wd.at[layer, span, :]))]

    finish_base = 1
    local_base = (0 if finish_layer is None else 1 + 3 * n_ff) + 4
    next_base = local_base + 3 * n_ff
    plan = []
    if finish_layer is not None:
        plan += [weight_copy(wo.at[finish_layer], 0)]
        plan += [copy for part in range(n_ff) for copy in ff_copies(finish_layer, finish_base, part)]
    if local_layer is not None:
        plan += [weight_copy(w.at[local_layer], local_base - 4 + which) for which, w in enumerate((wk, wv, wq, wo))]
        plan += [copy for part in range(n_ff) for copy in ff_copies(local_layer, local_base, part)]
        plan += [weight_copy(w.at[local_layer + 1], next_base + which) for which, w in enumerate((wq, wk, wv))]
    started = [0]

    def fetch(limit):
        for copy in plan[started[0]:limit]:
            copy.start()
        started[0] = max(started[0], min(limit, len(plan)))

    fetch(WINDOW)
    if local_layer is not None:
        x_send, x_halo, klt, vlt, keys, values, queries, attn_t, local_sem, halo_send, halo_recv = take(11)
        me = lax.axis_index('ctx')
        barrier = pltpu.get_barrier_semaphore()
        after, before = (me + 1) % n_dev, (me + n_dev - 1) % n_dev
        for neighbour in (after, before):
            pl.semaphore_signal(barrier, inc=1, device_id={'ctx': neighbour}, device_id_type=MESH_ID)
        pair = local_layer // 2
        local_copies = [pltpu.make_async_copy(kl_ref.at[pair], klt, local_sem.at[0]), pltpu.make_async_copy(vl_ref.at[pair], vlt, local_sem.at[1])]
        halo = pltpu.make_async_remote_copy(src_ref=x_ref if finish_layer is None else x_send, dst_ref=x_halo, send_sem=halo_send,
                                            recv_sem=halo_recv, device_id={'ctx': after}, device_id_type=MESH_ID)
        for copy in local_copies:
            copy.start()
        if finish_layer is None:
            pl.semaphore_wait(barrier, 2)
            halo.start()

    def block(at):
        fetch(at + WINDOW)
        plan[at].wait()
        return blocks[at]

    def mlp(hidden, layer, base):
        fetch(base + 3 * n_ff)
        rows_ref[...] = rms_rows(hidden, gm_ref[layer:layer + 1, :])
        sums[...] = hidden.astype(jnp.float32)

        def activate(part):
            gate_pre = mat(rows_ref[...], blocks[base + 3 * part])
            up_pre = mat(rows_ref[...], blocks[base + 3 * part + 1])
            acts[part % 2] = (jax.nn.gelu(gate_pre, approximate=True) * up_pre).astype(jnp.bfloat16)

        def shrink(part):
            sums[...] += mat(acts[part % 2], blocks[base + 3 * part + 2])

        def arrive(part):
            for copy in ff_copies(layer, base, part):
                copy.wait()

        arrive(0)
        activate(0)

        def step(part, carry):
            arrive(part)
            shrink(part - 1)
            activate(part)
            return carry

        lax.fori_loop(1, n_ff, step, 0)
        fetch(base + 3 * n_ff + WINDOW)
        shrink(n_ff - 1)
        return sums[...].astype(jnp.bfloat16)

    hidden = x_ref[...]
    if finish_layer is not None:
        attn = o_ref[...].T
        hidden = (hidden.astype(jnp.float32) + mat(attn, block(0))).astype(jnp.bfloat16)
        hidden = mlp(hidden, finish_layer, finish_base)
    if local_layer is None:
        y_ref[...] = hidden
        return
    if finish_layer is not None:
        x_send[...] = hidden
        pl.semaphore_wait(barrier, 2)
        halo.start()

    heads, head_dim = kl_ref.shape[1], kl_ref.shape[2]
    at = local_base - 4
    gain = ga_ref[local_layer:local_layer + 1, :]
    rows_ref[...] = rms_rows(hidden, gain)
    key_block = block(at)
    keys[n_rows:, :] = mat(rows_ref[...], key_block).astype(jnp.bfloat16)
    value_block = block(at + 1)
    values[:, n_rows:] = mat(rows_ref[...], value_block).astype(jnp.bfloat16).T
    queries[...] = mat(rows_ref[...], block(at + 2)).astype(jnp.bfloat16).T
    for copy in local_copies:
        copy.wait()
    fetch(at + 4 + WINDOW)
    first = me == 0
    halo.wait_recv()
    rows_ref[...] = rms_rows(x_halo[...], gain)
    keys[:n_rows, :] = jnp.where(first, klt[...].reshape(width, n_rows).T, mat(rows_ref[...], blocks[at]).astype(jnp.bfloat16))
    values[:, :n_rows] = jnp.where(first, vlt[...].reshape(width, n_rows), mat(rows_ref[...], blocks[at + 1]).astype(jnp.bfloat16).T)
    ahead = lax.broadcasted_iota(jnp.int32, (2 * n_rows, n_rows), 0) - lax.broadcasted_iota(jnp.int32, (2 * n_rows, n_rows), 1)
    seen = (ahead > 0) & (ahead <= n_rows)
    row = lax.broadcasted_iota(jnp.int32, (2 * head_dim, n_rows), 0)

    def head_pair(pair_at, carry):
        lanes = pl.ds(pl.multiple_of(2 * head_dim * pair_at, 2 * head_dim), 2 * head_dim)
        for half in range(2):
            columns = jnp.where(row // head_dim == half, queries[lanes, :], 0.0).astype(jnp.bfloat16)
            block_scores = mat(keys[:, lanes], columns) * (LOG2E * head_dim ** -0.5)
            block_scores = jnp.where(seen, block_scores, NEG)
            probs = jnp.exp2(block_scores - jnp.max(block_scores, axis=0, keepdims=True))
            below = jnp.sum(probs, axis=0, keepdims=True)
            rows = pl.ds(pl.multiple_of(2 * head_dim * pair_at + half * head_dim, head_dim), head_dim)
            attn_t[rows, :] = (mat(values[rows, :], probs.astype(jnp.bfloat16)) / below).astype(jnp.bfloat16)
        return carry

    lax.fori_loop(0, heads // 2, head_pair, 0)
    hidden = (hidden.astype(jnp.float32) + mat(attn_t[...].T, block(at + 3))).astype(jnp.bfloat16)
    hidden = mlp(hidden, local_layer, local_base)
    y_ref[...] = hidden
    rows_ref[...] = rms_rows(hidden, ga_ref[local_layer + 1:local_layer + 2, :])
    fetch(len(plan))

    def project(which, carry):
        weight_copy(wq.at[local_layer + 1], next_base + which).wait()
        qkv_ref[which] = mat(rows_ref[...], blocks[next_base + which]).astype(jnp.bfloat16).T.reshape(qkv_ref.shape[1:])
        return carry

    lax.fori_loop(0, 3, project, 0)
    halo.wait_send()


def dense(finish_layer, local_layer, n_dev, x_rows, gains, attn_t, weights, local_t):
    n_rows, width = x_rows.shape
    n_ff = weights[4].shape[2] // width
    vmem = pl.BlockSpec(memory_space=pltpu.VMEM)
    hbm = pl.BlockSpec(memory_space=pl.ANY)
    bf16 = jnp.bfloat16
    n_blocks = (0 if finish_layer is None else 1 + 3 * n_ff) + (0 if local_layer is None else 7 + 3 * n_ff)
    args, in_specs = [x_rows, *gains], [vmem] * 3
    out_shape, out_specs = [jax.ShapeDtypeStruct(x_rows.shape, bf16)], [vmem]
    scratch = [pltpu.VMEM((n_blocks, width, width), bf16), pltpu.SemaphoreType.DMA((n_blocks,)),
               pltpu.VMEM(x_rows.shape, bf16), pltpu.VMEM((2, *x_rows.shape), bf16), pltpu.VMEM(x_rows.shape, jnp.float32)]
    if finish_layer is not None:
        args.append(attn_t)
        in_specs.append(vmem)
    args += weights
    in_specs += [hbm] * len(weights)
    params = {}
    if local_layer is not None:
        args += local_t
        in_specs += [hbm] * 2
        _, heads, head_dim, window = local_t[0].shape
        out_shape += [jax.ShapeDtypeStruct((3, heads, head_dim, n_rows), bf16)]
        out_specs += [vmem]
        scratch += [pltpu.VMEM(x_rows.shape, bf16), pltpu.VMEM(x_rows.shape, bf16),
                    pltpu.VMEM((heads, head_dim, window), bf16), pltpu.VMEM((heads, head_dim, window), bf16),
                    pltpu.VMEM((window + n_rows, width), bf16), pltpu.VMEM((width, window + n_rows), bf16),
                    pltpu.VMEM((width, n_rows), bf16), pltpu.VMEM((width, n_rows), bf16),
                    pltpu.SemaphoreType.DMA((2,)), pltpu.SemaphoreType.DMA, pltpu.SemaphoreType.DMA]
        params = dict(collective_id=8 + local_layer, has_side_effects=True)
    return pl.pallas_call(
        functools.partial(dense_kernel, finish_layer, local_layer, n_dev),
        out_shape=tuple(out_shape), in_specs=in_specs, out_specs=tuple(out_specs), scratch_shapes=scratch,
        compiler_params=pltpu.CompilerParams(vmem_limit_bytes=60 * 2 ** 20, **params),
        name='dense_%s_%s' % (finish_layer, local_layer),
    )(*args)


def solution(mesh):
    ctx_size = mesh.shape['ctx']
    row_spec = P(('dp', 'ctx'), None)
    cache_spec = P(None, ('dp', 'ctx'), None, None)
    local_spec = P(None, 'dp', None, None)
    in_specs = (row_spec, P('dp'), cache_spec, cache_spec, local_spec, local_spec) + (P(),) * 9

    def device_step(x_rows, cache_len, k_cache, v_cache, k_local, v_local, g_attn, g_mlp, *weights):
        by_slot = lambda array: jnp.transpose(array, (0, 2, 3, 1))
        cache_t = [by_slot(k_cache), by_slot(v_cache)]
        local_t = [by_slot(k_local), by_slot(v_local)]
        gains = [g_attn, g_mlp]
        hidden, finish_layer, attn_t = x_rows, None, None
        for pair in range(k_cache.shape[0]):
            hidden, qkv = dense(finish_layer, 2 * pair, ctx_size, hidden, gains, attn_t, weights, local_t)
            attn_t = global_attention(pair, ctx_size, cache_len, qkv, *cache_t)
            attn_t = attn_t.reshape(-1, attn_t.shape[-1])
            finish_layer = 2 * pair + 1
        return dense(finish_layer, None, ctx_size, hidden, gains, attn_t, weights, local_t)[0]

    return jax.shard_map(device_step, mesh=mesh, in_specs=in_specs, out_specs=row_spec, check_vma=False)
```

```python
import functools

import jax
import jax.numpy as jnp
from jax import lax
from jax.experimental import pallas as pl
from jax.experimental.pallas import tpu as pltpu
from jax.sharding import PartitionSpec as P

NORM_EPS = 1e-6
WINDOW = 4
LOG2E = 1.4426950408889634
NEG = -1e38
MESH_ID = pl.DeviceIdType.MESH
ROWS = 256
SCORE_KEYS = 1152
VALUE_KEYS = 128
STATS = 8


def rms_rows(rows_in, gain_row):
    rows_f32 = rows_in.astype(jnp.float32)
    inv_rms = lax.rsqrt(jnp.mean(rows_f32 * rows_f32, axis=-1, keepdims=True) + NORM_EPS)
    return (rows_f32 * inv_rms * gain_row.astype(jnp.float32)).astype(jnp.bfloat16)


def mat(rows_in, weight):
    return jnp.dot(rows_in, weight, preferred_element_type=jnp.float32)


def ff_copies(weights, blocks, block_sem, layer, base, part):
    wg, wu, wd = weights
    width = wd.shape[2]
    span = pl.ds(pl.multiple_of(part * width, width), width)
    return [pltpu.make_async_copy(source, blocks.at[base + 3 * part + which], block_sem.at[base + 3 * part + which])
            for which, source in enumerate((wg.at[layer, :, span], wu.at[layer, :, span], wd.at[layer, span, :]))]


def mlp_rows(hidden, gain, n_ff, blocks, base, arrive, rows_ref, acts, sums):
    rows_ref[...] = rms_rows(hidden, gain)
    sums[...] = hidden.astype(jnp.float32)

    def activate(part):
        gate_pre = mat(rows_ref[...], blocks[base + 3 * part])
        up_pre = mat(rows_ref[...], blocks[base + 3 * part + 1])
        acts[part % 2] = (jax.nn.gelu(gate_pre, approximate=True) * up_pre).astype(jnp.bfloat16)

    def shrink(part):
        sums[...] += mat(acts[part % 2], blocks[base + 3 * part + 2])

    arrive(0)
    activate(0)

    def step(part, carry):
        arrive(part)
        shrink(part - 1)
        activate(part)
        return carry

    lax.fori_loop(1, n_ff, step, 0)
    shrink(n_ff - 1)
    return sums[...].astype(jnp.bfloat16)


def slot_of(step, head, n_slots):
    place = jnp.where(head == 0, step, n_slots - 1 - step)
    unit = place // 2
    return unit + unit // 2 - 2 * (unit // 3), place % 2


def global_kernel(n_chips, pair, len_ref, qkv_ref, x_ref, gm_ref, wo, wg, wu, wd, kc_ref, vc_ref, y_ref,
                  k_own, v_own, k_sib, v_sib, kn_sib, vn_sib, q_all, k_twice, k_mask, scores, part, parts,
                  blocks, block_sem, rows_ref, acts, sums, attn_t,
                  own_sem, sib_send, sib_recv, q_send, q_recv, o_send, o_recv):
    q_ref, k_ref, v_ref = qkv_ref.at[0], qkv_ref.at[1], qkv_ref.at[2]
    heads, head_dim, slots = k_own.shape
    n_slots = 2 * n_chips
    me = lax.axis_index('ctx')
    chip, core = me // 2, me % 2
    first_head = heads * core
    other_head = heads * (1 - core)
    sibling = {'ctx': 2 * chip + (1 - core)}
    n_new = 2 * ROWS
    n_keys = 2 * slots + n_new

    barrier = pltpu.get_barrier_semaphore()
    for step in range(1, n_slots):
        pl.semaphore_signal(barrier, inc=1, device_id={'ctx': (me + step) % n_slots}, device_id_type=MESH_ID)

    def own_copies(head):
        return (pltpu.make_async_copy(kc_ref.at[pair, first_head + head], k_own.at[head], own_sem.at[0, head]),
                pltpu.make_async_copy(vc_ref.at[pair, first_head + head], v_own.at[head], own_sem.at[1, head]))

    def sib_copies(head):
        pairs = ((kc_ref.at[pair, other_head + head], k_sib.at[head]),
                 (vc_ref.at[pair, other_head + head], v_sib.at[head]),
                 (k_ref.at[other_head + head], kn_sib.at[head]),
                 (v_ref.at[other_head + head], vn_sib.at[head]))
        return [pltpu.make_async_remote_copy(src_ref=src, dst_ref=dst, send_sem=sib_send.at[which, head],
                                             recv_sem=sib_recv.at[which, head], device_id=sibling, device_id_type=MESH_ID)
                for which, (src, dst) in enumerate(pairs)]

    def target(dist, flip):
        return {'ctx': 2 * ((chip + dist) % n_chips) + (core + flip) % 2}

    def q_copy(dist, flip, head):
        slot = 2 * dist + flip
        their_head = heads * ((core + flip) % 2) + head
        return pltpu.make_async_remote_copy(src_ref=q_ref.at[their_head], dst_ref=q_all.at[slot, head],
                                            send_sem=q_send.at[slot, head], recv_sem=q_recv.at[slot, head],
                                            device_id=target(dist, flip), device_id_type=MESH_ID)

    def o_copy(dist, flip, head):
        slot = 2 * dist + flip
        owner = {'ctx': 2 * ((chip + n_chips - dist) % n_chips) + (core + flip) % 2}
        return pltpu.make_async_remote_copy(src_ref=part.at[slot, head], dst_ref=parts.at[slot, head],
                                            send_sem=o_send.at[slot, head], recv_sem=o_recv.at[slot, head],
                                            device_id=owner, device_id_type=MESH_ID)

    def start_own(head, carry):
        for copy in own_copies(head):
            copy.start()
        q_all[0, head] = q_ref[first_head + head]
        return carry

    lax.fori_loop(0, heads, start_own, 0)
    pl.semaphore_wait(barrier, n_slots - 1)

    def start_head(head, carry):
        for copy in sib_copies(head):
            copy.start()

        def start_q(step, inner):
            dist, flip = slot_of(step, 0, n_slots)
            q_copy(dist, flip, head).start()
            return inner

        lax.fori_loop(1, n_slots, start_q, 0)
        return carry

    lax.fori_loop(0, heads, start_head, 0)

    layer = 2 * pair + 1
    n_rows, width = x_ref.shape
    n_ff = wg.shape[2] // width
    out_copy = pltpu.make_async_copy(wo.at[layer], blocks.at[0], block_sem.at[0])

    def mlp_copies(part):
        return ff_copies((wg, wu, wd), blocks, block_sem, layer, 1, part)

    valid = len_ref[0]

    def prepare(head):
        for copy in own_copies(head):
            copy.wait()
        for copy in sib_copies(head):
            copy.wait_recv()
        width = 512
        row = lax.broadcasted_iota(jnp.int32, (head_dim, width), 0)
        col = lax.broadcasted_iota(jnp.int32, (head_dim, width), 1)
        for begin in range(0, n_keys, width):
            if begin < 2 * slots:
                source = k_own if begin < slots else k_sib
                at = begin % slots
                tile = source[head, :, at:at + width]
                device = me if begin < slots else 2 * chip + (1 - core)
                bias = jnp.where((row == 0) & (device * slots + at + col >= valid), NEG, 0.0)
            else:
                tile = jnp.concatenate([k_ref[first_head + head], kn_sib[head]], axis=1)
                bias = jnp.where((row == 1) & (col < ROWS) | (row == 2) & (col >= ROWS), 1.0, 0.0)
            buf = head % 2
            k_twice[buf, begin:begin + width, :] = jnp.concatenate([tile, tile], axis=0).T
            k_mask[buf, begin:begin + width, :] = jnp.concatenate([tile, bias.astype(jnp.bfloat16)], axis=0).T

    def query_columns(head, dist, flip):
        slot = 2 * dist + flip
        full = q_all[slot, head].astype(jnp.float32) * (LOG2E * head_dim ** -0.5)
        high = full.astype(jnp.bfloat16)
        rest = full - high.astype(jnp.float32)
        middle = rest.astype(jnp.bfloat16)
        low = (rest - middle.astype(jnp.float32)).astype(jnp.bfloat16)
        q_dev = 2 * ((chip + n_chips - dist) % n_chips) + (core + flip) % 2
        row = lax.broadcasted_iota(jnp.int32, (head_dim, ROWS), 0)
        hide_own = jnp.where(q_dev < me, NEG, 0.0)
        hide_sib = jnp.where(q_dev < 2 * chip + (1 - core), NEG, 0.0)
        mask = jnp.where(row == 0, 1.0, jnp.where(row == 1, hide_own, jnp.where(row == 2, hide_sib, 0.0)))
        return jnp.concatenate([high, middle, low, mask.astype(jnp.bfloat16)], axis=0), q_dev

    def score_chunk(buf, columns, q_dev, begin, top):
        keys = pl.ds(begin, SCORE_KEYS)
        rows = jnp.concatenate([k_twice[buf, keys, :], k_mask[buf, keys, :]], axis=1)
        block = jnp.dot(rows, columns, preferred_element_type=jnp.float32)
        plain = min(max(2 * slots - begin, 0), SCORE_KEYS)
        pieces = [block[:plain]] if plain else []
        for at in range(plain, SCORE_KEYS, ROWS):
            device = me if begin + at < 2 * slots + ROWS else 2 * chip + (1 - core)
            ahead = lax.broadcasted_iota(jnp.int32, (ROWS, ROWS), 0) - lax.broadcasted_iota(jnp.int32, (ROWS, ROWS), 1)
            pieces.append(jnp.where(ahead <= jnp.where(q_dev == device, 0, ROWS), block[at:at + ROWS], NEG))
        at = begin
        for piece in pieces:
            scores[pl.ds(at, piece.shape[0]), :] = piece
            top = jnp.maximum(top, jnp.max(piece.reshape(piece.shape[0] // 8, 8, ROWS), axis=0))
            at += piece.shape[0]
        return top

    def value_chunk(head, base, begin, total, weighted):
        probs = jnp.exp2(scores[pl.ds(begin, VALUE_KEYS), :] - base)
        total = total + jnp.sum(probs.reshape(VALUE_KEYS // 8, 8, ROWS), axis=0)
        if begin < slots:
            values = v_own[head, :, begin:begin + VALUE_KEYS]
        elif begin < 2 * slots:
            values = v_sib[head, :, begin - slots:begin - slots + VALUE_KEYS]
        elif begin < 2 * slots + ROWS:
            values = v_ref[first_head + head, :, begin - 2 * slots:begin - 2 * slots + VALUE_KEYS]
        else:
            values = vn_sib[head, :, begin - 2 * slots - ROWS:begin - 2 * slots - ROWS + VALUE_KEYS]
        return total, weighted + jnp.dot(values, probs.astype(jnp.bfloat16), preferred_element_type=jnp.float32)

    order = sorted([(begin + VALUE_KEYS, 0, begin) for begin in range(0, n_keys, VALUE_KEYS)]
                   + [(begin + SCORE_KEYS, 1, begin) for begin in range(0, n_keys, SCORE_KEYS)])
    no_top = jnp.full((8, ROWS), NEG, jnp.float32)

    prepare(0)
    out_copy.start()
    for part_at in range(n_ff):
        for copy in mlp_copies(part_at):
            copy.start()
    columns, q_dev = query_columns(0, 0, 0)
    top = no_top
    for begin in range(0, n_keys, SCORE_KEYS):
        top = score_chunk(0, columns, q_dev, begin, top)

    def one_head(head, top):
        next_head = jnp.minimum(head + 1, heads - 1)

        @pl.when(head < heads - 1)
        def _():
            prepare(next_head)

        def one_step(step, top):
            dist, flip = slot_of(step, head, n_slots)
            slot = 2 * dist + flip
            after = (step + 1) % n_slots
            head_n = jnp.where(step == n_slots - 1, next_head, head)
            dist_n, flip_n = slot_of(after, head_n, n_slots)
            remote_n = (2 * dist_n + flip_n > 0) & ((step < n_slots - 1) | (head < heads - 1))

            @pl.when(remote_n)
            def _():
                q_copy(dist_n, flip_n, head_n).wait_recv()

            columns, q_dev = query_columns(head_n, dist_n, flip_n)
            base = jnp.max(top, axis=0, keepdims=True)
            total = jnp.zeros((8, ROWS), jnp.float32)
            weighted = jnp.zeros((head_dim, ROWS), jnp.float32)
            new_top = no_top
            for _, kind, begin in order:
                if kind == 0:
                    total, weighted = value_chunk(head, base, begin, total, weighted)
                else:
                    new_top = score_chunk(head_n % 2, columns, q_dev, begin, new_top)
            row = lax.broadcasted_iota(jnp.int32, (STATS, ROWS), 0)
            total = jnp.sum(total, axis=0, keepdims=True)
            part[slot, head, 0:head_dim, :] = weighted
            part[slot, head, head_dim:, :] = jnp.where(row == 0, base, total)

            @pl.when(slot > 0)
            def _():
                o_copy(dist, flip, head).start()

            return new_top

        return lax.fori_loop(0, n_slots, one_step, top)

    lax.fori_loop(0, heads, one_head, top)

    def merge(head, carry):
        for flip in range(2):
            found = []
            for dist in range(n_chips):
                slot = 2 * dist + flip
                if slot == 0:
                    found.append((part[0, head, 0:head_dim, :], part[0, head, head_dim:head_dim + 1, :],
                                  part[0, head, head_dim + 1:head_dim + 2, :]))
                else:
                    o_copy(dist, flip, head).wait_recv()
                    found.append((parts[slot, head, 0:head_dim, :], parts[slot, head, head_dim:head_dim + 1, :],
                                  parts[slot, head, head_dim + 1:head_dim + 2, :]))
            peak = functools.reduce(jnp.maximum, [base for _, base, _ in found])
            scaled = [(weighted, total, jnp.exp2(base - peak)) for weighted, base, total in found]
            upper = sum(weighted * factor for weighted, _, factor in scaled)
            lower = sum(total * factor for _, total, factor in scaled)
            attn_t[heads * ((core + flip) % 2) + head] = (upper / lower).astype(jnp.bfloat16)
        return carry

    lax.fori_loop(0, heads, merge, 0)
    out_copy.wait()
    attn = attn_t[...].reshape(width, n_rows).T
    hidden = (x_ref[...].astype(jnp.float32) + mat(attn, blocks[0])).astype(jnp.bfloat16)

    def arrive(part_at):
        for copy in mlp_copies(part_at):
            copy.wait()

    y_ref[...] = mlp_rows(hidden, gm_ref[layer:layer + 1, :], n_ff, blocks, 1, arrive, rows_ref, acts, sums)

    def finish(head, carry):
        for copy in sib_copies(head):
            copy.wait_send()

        def finish_step(step, inner):
            dist, flip = slot_of(step, 0, n_slots)
            q_copy(dist, flip, head).wait_send()
            o_copy(dist, flip, head).wait_send()
            return inner

        lax.fori_loop(1, n_slots, finish_step, 0)
        return carry

    lax.fori_loop(0, heads, finish, 0)


def global_layer(pair, n_dev, valid_len, qkv, x_rows, mlp_gain, weights, cache_k, cache_v):
    _, all_heads, head_dim, rows = qkv.shape
    heads = all_heads // 2
    slots = cache_k.shape[-1]
    n_keys = 2 * (slots + rows)
    width = x_rows.shape[1]
    n_blocks = 1 + 3 * (weights[1].shape[2] // width)
    vmem = pl.BlockSpec(memory_space=pltpu.VMEM)
    bf16, f32 = jnp.bfloat16, jnp.float32
    return pl.pallas_call(
        functools.partial(global_kernel, n_dev // 2, pair),
        out_shape=jax.ShapeDtypeStruct(x_rows.shape, bf16),
        in_specs=[pl.BlockSpec(memory_space=pltpu.SMEM), vmem, vmem, vmem] + [pl.BlockSpec(memory_space=pl.ANY)] * 6,
        out_specs=vmem,
        scratch_shapes=[
            pltpu.VMEM((heads, head_dim, slots), bf16), pltpu.VMEM((heads, head_dim, slots), bf16),
            pltpu.VMEM((heads, head_dim, slots), bf16), pltpu.VMEM((heads, head_dim, slots), bf16),
            pltpu.VMEM((heads, head_dim, rows), bf16), pltpu.VMEM((heads, head_dim, rows), bf16),
            pltpu.VMEM((n_dev, heads, head_dim, rows), bf16),
            pltpu.VMEM((2, n_keys, 2 * head_dim), bf16), pltpu.VMEM((2, n_keys, 2 * head_dim), bf16),
            pltpu.VMEM((n_keys, rows), f32),
            pltpu.VMEM((n_dev, heads, head_dim + STATS, rows), f32),
            pltpu.VMEM((n_dev, heads, head_dim + STATS, rows), f32),
            pltpu.VMEM((n_blocks, width, width), bf16), pltpu.SemaphoreType.DMA((n_blocks,)),
            pltpu.VMEM(x_rows.shape, bf16), pltpu.VMEM((2, *x_rows.shape), bf16), pltpu.VMEM(x_rows.shape, f32),
            pltpu.VMEM((all_heads, head_dim, rows), bf16),
            pltpu.SemaphoreType.DMA((2, heads)),
            pltpu.SemaphoreType.DMA((4, heads)), pltpu.SemaphoreType.DMA((4, heads)),
            pltpu.SemaphoreType.DMA((n_dev, heads)), pltpu.SemaphoreType.DMA((n_dev, heads)),
            pltpu.SemaphoreType.DMA((n_dev, heads)), pltpu.SemaphoreType.DMA((n_dev, heads)),
        ],
        compiler_params=pltpu.CompilerParams(collective_id=pair, has_side_effects=True, vmem_limit_bytes=60 * 2 ** 20),
        name='global_%d' % pair,
    )(valid_len, qkv, x_rows, mlp_gain, *weights, cache_k, cache_v)


def local_kernel(layer, n_dev, x_ref, ga_ref, gm_ref, wq, wk, wv, wo, wg, wu, wd, kl_ref, vl_ref, y_ref, qkv_ref,
                 blocks, block_sem, rows_ref, acts, sums, x_halo, klt, vlt, keys, values, queries, attn_t,
                 local_sem, halo_send, halo_recv):
    n_rows, width = x_ref.shape
    n_ff = wg.shape[2] // width
    base, next_base = 4, 4 + 3 * n_ff

    def weight_copy(source, at):
        return pltpu.make_async_copy(source, blocks.at[at], block_sem.at[at])

    def mlp_copies(part):
        return ff_copies((wg, wu, wd), blocks, block_sem, layer, base, part)

    plan = [weight_copy(w.at[layer], which) for which, w in enumerate((wk, wv, wq, wo))]
    plan += [copy for part in range(n_ff) for copy in mlp_copies(part)]
    plan += [weight_copy(w.at[layer + 1], next_base + which) for which, w in enumerate((wq, wk, wv))]
    started = [0]

    def fetch(limit):
        for copy in plan[started[0]:limit]:
            copy.start()
        started[0] = max(started[0], min(limit, len(plan)))

    me = lax.axis_index('ctx')
    barrier = pltpu.get_barrier_semaphore()
    after, before = (me + 1) % n_dev, (me + n_dev - 1) % n_dev
    for neighbour in (after, before):
        pl.semaphore_signal(barrier, inc=1, device_id={'ctx': neighbour}, device_id_type=MESH_ID)
    fetch(WINDOW)
    pair = layer // 2
    local_copies = [pltpu.make_async_copy(kl_ref.at[pair], klt, local_sem.at[0]), pltpu.make_async_copy(vl_ref.at[pair], vlt, local_sem.at[1])]
    halo = pltpu.make_async_remote_copy(src_ref=x_ref, dst_ref=x_halo, send_sem=halo_send, recv_sem=halo_recv,
                                        device_id={'ctx': after}, device_id_type=MESH_ID)
    for copy in local_copies:
        copy.start()
    pl.semaphore_wait(barrier, 2)
    halo.start()

    def block(at):
        fetch(at + WINDOW)
        plan[at].wait()
        return blocks[at]

    hidden = x_ref[...]
    heads, head_dim = kl_ref.shape[1], kl_ref.shape[2]
    gain = ga_ref[layer:layer + 1, :]
    rows_ref[...] = rms_rows(hidden, gain)
    keys[n_rows:, :] = mat(rows_ref[...], block(0)).astype(jnp.bfloat16)
    values[:, n_rows:] = mat(rows_ref[...], block(1)).astype(jnp.bfloat16).T
    queries[...] = mat(rows_ref[...], block(2)).astype(jnp.bfloat16).T
    for copy in local_copies:
        copy.wait()
    fetch(len(plan))
    first = me == 0
    halo.wait_recv()
    rows_ref[...] = rms_rows(x_halo[...], gain)
    keys[:n_rows, :] = jnp.where(first, klt[...].reshape(width, n_rows).T, mat(rows_ref[...], blocks[0]).astype(jnp.bfloat16))
    values[:, :n_rows] = jnp.where(first, vlt[...].reshape(width, n_rows), mat(rows_ref[...], blocks[1]).astype(jnp.bfloat16).T)
    ahead = lax.broadcasted_iota(jnp.int32, (2 * n_rows, n_rows), 0) - lax.broadcasted_iota(jnp.int32, (2 * n_rows, n_rows), 1)
    seen = (ahead > 0) & (ahead <= n_rows)
    row = lax.broadcasted_iota(jnp.int32, (2 * head_dim, n_rows), 0)

    def head_pair(pair_at, carry):
        lanes = pl.ds(pl.multiple_of(2 * head_dim * pair_at, 2 * head_dim), 2 * head_dim)
        for half in range(2):
            columns = jnp.where(row // head_dim == half, queries[lanes, :], 0.0).astype(jnp.bfloat16)
            block_scores = mat(keys[:, lanes], columns) * (LOG2E * head_dim ** -0.5)
            block_scores = jnp.where(seen, block_scores, NEG)
            probs = jnp.exp2(block_scores - jnp.max(block_scores, axis=0, keepdims=True))
            below = jnp.sum(probs, axis=0, keepdims=True)
            rows = pl.ds(pl.multiple_of(2 * head_dim * pair_at + half * head_dim, head_dim), head_dim)
            attn_t[rows, :] = (mat(values[rows, :], probs.astype(jnp.bfloat16)) / below).astype(jnp.bfloat16)
        return carry

    lax.fori_loop(0, heads // 2, head_pair, 0)
    hidden = (hidden.astype(jnp.float32) + mat(attn_t[...].T, block(3))).astype(jnp.bfloat16)

    def arrive(part):
        for copy in mlp_copies(part):
            copy.wait()

    hidden = mlp_rows(hidden, gm_ref[layer:layer + 1, :], n_ff, blocks, base, arrive, rows_ref, acts, sums)
    y_ref[...] = hidden
    rows_ref[...] = rms_rows(hidden, ga_ref[layer + 1:layer + 2, :])

    def project(which, carry):
        weight_copy(wq.at[layer + 1], next_base + which).wait()
        qkv_ref[which] = mat(rows_ref[...], blocks[next_base + which]).astype(jnp.bfloat16).T.reshape(qkv_ref.shape[1:])
        return carry

    lax.fori_loop(0, 3, project, 0)
    halo.wait_send()


def local_layer(layer, n_dev, x_rows, gains, weights, local_t):
    n_rows, width = x_rows.shape
    n_ff = weights[4].shape[2] // width
    _, heads, head_dim, window = local_t[0].shape
    vmem = pl.BlockSpec(memory_space=pltpu.VMEM)
    hbm = pl.BlockSpec(memory_space=pl.ANY)
    bf16 = jnp.bfloat16
    n_blocks = 7 + 3 * n_ff
    return pl.pallas_call(
        functools.partial(local_kernel, layer, n_dev),
        out_shape=(jax.ShapeDtypeStruct(x_rows.shape, bf16), jax.ShapeDtypeStruct((3, heads, head_dim, n_rows), bf16)),
        in_specs=[vmem] * 3 + [hbm] * (len(weights) + 2), out_specs=(vmem, vmem),
        scratch_shapes=[
            pltpu.VMEM((n_blocks, width, width), bf16), pltpu.SemaphoreType.DMA((n_blocks,)),
            pltpu.VMEM(x_rows.shape, bf16), pltpu.VMEM((2, *x_rows.shape), bf16), pltpu.VMEM(x_rows.shape, jnp.float32),
            pltpu.VMEM(x_rows.shape, bf16),
            pltpu.VMEM((heads, head_dim, window), bf16), pltpu.VMEM((heads, head_dim, window), bf16),
            pltpu.VMEM((window + n_rows, width), bf16), pltpu.VMEM((width, window + n_rows), bf16),
            pltpu.VMEM((width, n_rows), bf16), pltpu.VMEM((width, n_rows), bf16),
            pltpu.SemaphoreType.DMA((2,)), pltpu.SemaphoreType.DMA, pltpu.SemaphoreType.DMA],
        compiler_params=pltpu.CompilerParams(collective_id=8 + layer, has_side_effects=True, vmem_limit_bytes=60 * 2 ** 20),
        name='local_%d' % layer,
    )(x_rows, *gains, *weights, *local_t)


def solution(mesh):
    ctx_size = mesh.shape['ctx']
    row_spec = P(('dp', 'ctx'), None)
    cache_spec = P(None, ('dp', 'ctx'), None, None)
    local_spec = P(None, 'dp', None, None)
    in_specs = (row_spec, P('dp'), cache_spec, cache_spec, local_spec, local_spec) + (P(),) * 9

    def device_step(x_rows, cache_len, k_cache, v_cache, k_local, v_local, g_attn, g_mlp, *weights):
        by_slot = lambda array: jnp.transpose(array, (0, 2, 3, 1))
        cache_t = [by_slot(k_cache), by_slot(v_cache)]
        local_t = [by_slot(k_local), by_slot(v_local)]
        gains = [g_attn, g_mlp]
        hidden = x_rows
        for pair in range(k_cache.shape[0]):
            hidden, qkv = local_layer(2 * pair, ctx_size, hidden, gains, weights, local_t)
            hidden = global_layer(pair, ctx_size, cache_len, qkv, hidden, g_mlp, weights[3:], *cache_t)
        return hidden

    return jax.shard_map(device_step, mesh=mesh, in_specs=in_specs, out_specs=row_spec, check_vma=False)
```
